32 devices in a mesh: dp: 2 (over x), tp: 4 (over z), sp: 4 (over y, core).
Axes of the slice: x: 2, y: 2, z: 4, core: 2. Of those that a mesh axis runs over, the one named last changes fastest.
Arguments:
- hidden: bfloat16 [128, 8192], P('dp'), parts along dimension 0
- norm_scale: bfloat16 [8192], replicated
- w_qkv: bfloat16 [8192, 10240], P(None, 'tp')
- w_out: bfloat16 [8192, 8192], P('tp')
- k_cache: bfloat16 [128, 1024, 8, 128], P('dp', 'sp', 'tp'), parts along dimension 0
- v_cache: bfloat16 [128, 1024, 8, 128], P('dp', 'sp', 'tp'), parts along dimension 0
- positions: int32 [128], P('dp'), parts along dimension 0
Outputs:
- output 1: bfloat16 [128, 8192], P('dp'), parts along dimension 0
- output 2: bfloat16 [128, 1024, 8, 128], P('dp', 'sp', 'tp'), parts along dimension 0
- output 3: bfloat16 [128, 1024, 8, 128], P('dp', 'sp', 'tp'), parts along dimension 0
There are 2 independent parts. The reference program is written for one: setup_inputs(seed, part) draws one part's arguments, and reference() takes and returns one part's arrays. A program takes and returns all parts, laid end to end along the dimension named above; an argument that names none is the same for every part.
All inputs are finite; a program needn't handle non-finite values.
Results may differ from the reference program's by a relative error of at most 0.00672219.
Values sent between devices are 32-bit elements.
A program may use at most 1 GiB of HBM per device.

```python
import math
import jax
import jax.numpy as jnp
from jax import lax

BATCH = 64
SEQ = 1024
D = 8192
HEADS = 64
KV_HEADS = 8
HEAD = 128


def rope_apply(head_vals, positions):
    half_dim = head_vals.shape[-1] // 2
    inv_freq = jnp.exp(jnp.arange(half_dim, dtype=jnp.float32) * (-2.0 * math.log(500000.0) / head_vals.shape[-1]))
    angles = positions.astype(jnp.float32)[:, None] * inv_freq[None, :]
    cos_part = jnp.cos(angles)[:, None, None, :]
    sin_part = jnp.sin(angles)[:, None, None, :]
    first_half = head_vals[..., :half_dim]
    second_half = head_vals[..., half_dim:]
    return jnp.concatenate([first_half * cos_part - second_half * sin_part, second_half * cos_part + first_half * sin_part], axis=-1)


def setup_inputs(seed: int = 0, part: int = 0) -> dict:
    part_keys = jax.random.split(jax.random.fold_in(jax.random.key(seed), part), 5)
    shared_keys = jax.random.split(jax.random.key(seed + 1), 4)
    qkv_width = (HEADS + 2 * KV_HEADS) * HEAD
    hidden = jax.random.normal(part_keys[0], (BATCH, D), jnp.float32)
    norm_scale = 1.0 + 0.5 * jax.random.normal(shared_keys[0], (D,), jnp.float32)
    col_boost = jnp.where(jax.random.randint(shared_keys[1], (qkv_width,), 0, 16) == 0, 10.0, 1.0)
    w_qkv = jax.random.normal(shared_keys[2], (D, qkv_width), jnp.float32) * col_boost * (D ** -0.5)
    w_out = jax.random.normal(shared_keys[3], (HEADS * HEAD, D), jnp.float32) * (2.0 * (HEADS * HEAD) ** -0.5)
    k_cache = 0.5 * jax.random.normal(part_keys[1], (BATCH, SEQ, KV_HEADS, HEAD), jnp.float32)
    coarse = jax.random.normal(part_keys[2], (BATCH, 8, 1, KV_HEADS, HEAD), jnp.float32)
    fine_part = jax.random.normal(part_keys[3], (BATCH, 8, SEQ // 8, KV_HEADS, HEAD), jnp.float32)
    v_cache = (coarse + 0.5 * fine_part).reshape(BATCH, SEQ, KV_HEADS, HEAD)
    positions = jax.random.randint(part_keys[4], (BATCH,), SEQ // 8, SEQ)
    positions = positions.at[0].set(SEQ - 1).at[1].set(SEQ // 8)
    return {
        'hidden': hidden.astype(jnp.bfloat16),
        'norm_scale': norm_scale.astype(jnp.bfloat16),
        'w_qkv': w_qkv.astype(jnp.bfloat16),
        'w_out': w_out.astype(jnp.bfloat16),
        'k_cache': k_cache.astype(jnp.bfloat16),
        'v_cache': v_cache.astype(jnp.bfloat16),
        'positions': positions.astype(jnp.int32),
    }


def reference(hidden, norm_scale, w_qkv, w_out, k_cache, v_cache, positions):
    q_per_kv = HEADS // KV_HEADS
    hidden_f32 = hidden.astype(jnp.float32)
    row_mean = jnp.mean(hidden_f32, axis=-1, keepdims=True)
    centered = hidden_f32 - row_mean
    row_var = jnp.mean(centered * centered, axis=-1, keepdims=True)
    normed = (centered * lax.rsqrt(row_var + 1e-5) * norm_scale.astype(jnp.float32)).astype(jnp.bfloat16)
    qkv_proj = jnp.clip(jnp.dot(normed, w_qkv, preferred_element_type=jnp.float32).astype(jnp.bfloat16), -8.0, 8.0)
    grouped = qkv_proj.reshape(BATCH, KV_HEADS, q_per_kv + 2, HEAD)
    rotated = rope_apply(grouped[:, :, : q_per_kv + 1].astype(jnp.float32), positions).astype(jnp.bfloat16)
    queries = rotated[:, :, :q_per_kv]
    new_row = (jnp.arange(SEQ)[None, :] == positions[:, None])[:, :, None, None]
    k_upd = jnp.where(new_row, rotated[:, :, q_per_kv][:, None], k_cache)
    v_upd = jnp.where(new_row, grouped[:, :, q_per_kv + 1][:, None], v_cache)

    def one_sequence(seq_args):
        q_seq, k_seq, v_seq, p_seq = seq_args
        scores = jnp.einsum('gqd,sgd->gqs', q_seq.astype(jnp.float32), k_seq.astype(jnp.float32)) * (HEAD ** -0.5)
        valid_mask = jnp.arange(SEQ) <= p_seq
        scores = jnp.where(valid_mask[None, None, :], scores, -jnp.inf)
        weights_bf = jax.nn.softmax(scores, axis=-1).astype(jnp.bfloat16)
        return jnp.einsum('gqs,sgd->gqd', weights_bf.astype(jnp.float32), v_seq.astype(jnp.float32))

    attn_out = lax.map(one_sequence, (queries, k_upd, v_upd, positions))
    attn_flat = attn_out.reshape(BATCH, HEADS * HEAD).astype(jnp.bfloat16)
    h_out = (hidden_f32 + jnp.dot(attn_flat, w_out, preferred_element_type=jnp.float32)).astype(jnp.bfloat16)
    return (h_out, k_upd, v_upd)
```

```python
import math
import jax
import jax.numpy as jnp
from jax import lax
from jax.experimental import pallas as pl
from jax.experimental.pallas import tpu as pltpu
from jax.sharding import PartitionSpec as P

F32 = jnp.float32
BF16 = jnp.bfloat16
HD = 128
NEG = -3e38
FLOOR = -1e38
MESH_ID = pl.DeviceIdType.MESH
CHUNK = 128


def rope_tables(positions):
    half_dim = HD // 2
    inv_freq = jnp.exp(jnp.arange(half_dim, dtype=F32) * (-2.0 * math.log(500000.0) / HD))
    angles = positions.astype(F32)[:, None] * inv_freq[None, :]
    cos_part, sin_part = jnp.cos(angles), jnp.sin(angles)
    return jnp.concatenate([cos_part, cos_part], axis=-1), jnp.concatenate([-sin_part, sin_part], axis=-1)


def remote(src, dst, send_sem, recv_sem, device_id):
    return pltpu.make_async_remote_copy(
        src_ref=src, dst_ref=dst, send_sem=send_sem, recv_sem=recv_sem, device_id=device_id, device_id_type=MESH_ID
    )


def sp_peers():
    sp = lax.axis_index('sp')
    return sp, sp + 1 - 2 * lax.rem(sp, 2), lax.rem(sp + 2, 4)


def enter(peers):
    barrier = pltpu.get_barrier_semaphore()
    for peer in peers:
        pl.semaphore_signal(barrier, inc=1, device_id=peer, device_id_type=MESH_ID)
    pl.semaphore_wait(barrier, len(peers))


def qkv_kernel(h_ref, scale_ref, cos_ref, sin_ref, w_hbm, kc_hbm, vc_hbm, qkv_ref, k_ref, v_ref,
               w_buf, u_ref, w_sem, c_sem, send_sem, recv_sem):
    sp, partner, cross = sp_peers()
    width = w_buf.shape[1]
    heads = width // HD
    pieces = w_sem.shape[0]
    depth = w_buf.shape[0] // pieces
    col = pl.multiple_of(sp * width, HD)
    w_copies = [
        pltpu.make_async_copy(w_hbm.at[pl.ds(i * depth, depth), pl.ds(col, width)], w_buf.at[pl.ds(i * depth, depth)], w_sem.at[i])
        for i in range(pieces)
    ]
    for copy in w_copies:
        copy.start()
    enter([{'sp': partner}, {'sp': cross}])

    d = h_ref.shape[1]
    x = h_ref[...].astype(F32)
    mean = jnp.sum(x, axis=-1, keepdims=True) * (1.0 / d)
    centered = x - mean
    var = jnp.sum(centered * centered, axis=-1, keepdims=True) * (1.0 / d)
    inv = lax.rsqrt(var + 1e-5)
    u_ref[...] = ((h_ref[...].astype(F32) - mean) * inv * scale_ref[...].astype(F32)).astype(BF16)

    cache_copies = [pltpu.make_async_copy(kc_hbm, k_ref, c_sem.at[0]), pltpu.make_async_copy(vc_hbm, v_ref, c_sem.at[1])]
    acc = None
    for i in range(pieces):
        w_copies[i].wait()
        if i == pieces // 2:
            cache_copies[0].start()
        part = jnp.dot(u_ref[:, i * depth:(i + 1) * depth], w_buf[i * depth:(i + 1) * depth, :], preferred_element_type=F32)
        acc = part if acc is None else acc + part
    cache_copies[1].start()
    proj = jnp.clip(acc.astype(BF16).astype(F32), -8.0, 8.0)
    odd = lax.rem(sp, 2)
    for j in range(heads):
        val = proj[:, j * HD:(j + 1) * HD]
        rot = (val * cos_ref[...] + pltpu.roll(val, HD // 2, 1) * sin_ref[...]).astype(BF16).astype(F32)
        if j == heads - 1:
            rot = jnp.where(odd == 1, val, rot)
        qkv_ref[sp, j] = rot
    to_partner = remote(qkv_ref.at[sp], qkv_ref.at[sp], send_sem.at[0], recv_sem.at[0], {'sp': partner})
    to_cross = remote(qkv_ref.at[sp], qkv_ref.at[sp], send_sem.at[1], recv_sem.at[1], {'sp': cross})
    to_cross.start()
    to_partner.start()
    to_cross.wait_recv()
    forward = remote(qkv_ref.at[cross], qkv_ref.at[cross], send_sem.at[2], recv_sem.at[2], {'sp': partner})
    forward.start()
    to_partner.wait()
    to_cross.wait_send()
    forward.wait()
    for copy in cache_copies:
        copy.wait()


def attention_kernel(pos_ref, qkv_ref, k_ref, v_ref, k_out, v_out, acc_ref, stat_ref, q_ref, out_sem):
    n_seq, rows, _ = k_ref.shape
    seq_local = rows // 2
    group = acc_ref.shape[2]
    base = lax.axis_index('sp') * seq_local
    per_kv = group + 2
    for g in range(2):
        for j in range(group):
            n = g * per_kv + j
            q_ref[pl.ds(g * group + j, n_seq, stride=2 * group), :] = qkv_ref[n]

    tile = 16
    row_id = lax.broadcasted_iota(jnp.int32, (tile, HD), 0)

    def patch(b, carry):
        row = 2 * (pos_ref[b] - base)

        @pl.when((row >= 0) & (row < rows))
        def _():
            start = pl.multiple_of((row // tile) * tile, tile)
            off = row - start
            for ref, slot in ((k_ref, group), (v_ref, group + 1)):
                block = ref[b, pl.ds(start, tile), :].astype(F32)
                first = qkv_ref[slot, pl.ds(b, 1), :]
                second = qkv_ref[per_kv + slot, pl.ds(b, 1), :]
                block = jnp.where(row_id == off, first, jnp.where(row_id == off + 1, second, block))
                ref[b, pl.ds(start, tile), :] = block.astype(BF16)

        return carry

    lax.fori_loop(0, n_seq, patch, 0)
    pieces = out_sem.shape[1]
    span = n_seq // pieces
    copies = []
    for i in range(pieces):
        for s, (src, dst) in enumerate(((k_ref, k_out), (v_ref, v_out))):
            copy = pltpu.make_async_copy(src.at[pl.ds(i * span, span)], dst.at[pl.ds(i * span, span)], out_sem.at[s, i])
            copy.start()
            copies.append(copy)

    n_q = 2 * group
    col_id = lax.broadcasted_iota(jnp.int32, (n_q, rows), 1)
    head_id = lax.broadcasted_iota(jnp.int32, (n_q, rows), 0) // group
    col_key = jnp.where(lax.rem(col_id, 2) == head_id, col_id, 1 << 30)
    lane = lax.broadcasted_iota(jnp.int32, (n_q, HD), 1)
    factor = HD ** -0.5 * math.log2(math.e)
    unroll = 4

    def step(i, stats):
        results = []
        for r in range(unroll):
            b = i * unroll + r
            limit = 2 * (pos_ref[b] - base + 1)
            q = q_ref[pl.ds(pl.multiple_of(b * n_q, n_q), n_q), :].astype(BF16)
            scores = lax.dot_general(q, k_ref[b], (((1,), (1,)), ((), ())), preferred_element_type=F32) * factor
            scores = jnp.where(col_key < limit, scores, NEG)
            top = jnp.maximum(jnp.max(scores, axis=-1, keepdims=True), FLOOR)
            probs = jnp.exp2(scores - top)
            total = jnp.sum(probs, axis=-1, keepdims=True)
            out = jnp.dot(probs.astype(BF16), v_ref[b], preferred_element_type=F32)
            results.append((b, top, total, out))
        for b, top, total, out in results:
            acc_ref[0, b] = out[:group]
            acc_ref[1, b] = out[group:]
            stats = jnp.where(lane == b, top, jnp.where(lane == b + n_seq, total, stats))
        return stats

    stats = lax.fori_loop(0, n_seq // unroll, step, jnp.zeros((n_q, HD), F32))
    stat_ref[0] = stats[:group]
    stat_ref[1] = stats[group:]
    for copy in copies:
        copy.wait()


def project_kernel(h_ref, acc_ref, stat_ref, w_hbm, out_ref, w_buf, d_acc, d_stat, m_acc, m_stat, y_acc, y_stat, att, a_ref,
                   part, e_buf, a_buf, b_buf, tot, y_buf, p1_buf, p2_buf,
                   w_sem, st_send, st_recv, d_send, d_recv, y_send, y_recv, g_send, g_recv,
                   e_send, e_recv, b_send, b_recv, t_send, t_recv, ys, yr, p1s, p1r, p2s, p2r):
    sp, partner, cross = sp_peers()
    core = lax.rem(sp, 2)
    z = lax.axis_index('tp')
    is_hub = (z == 1) | (z == 2)
    end_of_hub = 3 * (z - 1)
    hub_of_end = 1 + z // 2
    other_hub = 3 - z
    n_seq = h_ref.shape[0]
    width = w_buf.shape[1]
    col = pl.multiple_of(sp * width, HD)
    w_copy = pltpu.make_async_copy(w_hbm.at[:, pl.ds(col, width)], w_buf, w_sem)
    w_copy.start()

    barrier = pltpu.get_barrier_semaphore()
    for peer in ({'sp': partner}, {'sp': cross}):
        pl.semaphore_signal(barrier, inc=1, device_id=peer, device_id_type=MESH_ID)

    @pl.when(is_hub)
    def _():
        for peer in ({'tp': end_of_hub}, {'tp': other_hub}):
            pl.semaphore_signal(barrier, inc=1, device_id=peer, device_id_type=MESH_ID)
        pl.semaphore_wait(barrier, 4)

    @pl.when(jnp.logical_not(is_hub))
    def _():
        pl.semaphore_signal(barrier, inc=1, device_id={'tp': hub_of_end}, device_id_type=MESH_ID)
        pl.semaphore_wait(barrier, 3)

    group = stat_ref.shape[1]
    blocks = d_send.shape[0]
    span = n_seq // blocks
    height = span * group
    other = 1 - core
    st_copy = remote(stat_ref.at[other], d_stat, st_send.at[0], st_recv.at[0], {'sp': partner})
    st_copy.start()
    d_copies = []
    for i in range(blocks):
        copy = remote(acc_ref.at[other, pl.ds(i * height, height)], d_acc.at[pl.ds(i * height, height)],
                      d_send.at[i], d_recv.at[i], {'sp': partner})
        copy.start()
        d_copies.append(copy)
    st_copy.wait_recv()
    lane = lax.broadcasted_iota(jnp.int32, (group, HD), 1)

    def weights(s0, s1):
        l0, l1 = pltpu.roll(s0, HD // 2, 1), pltpu.roll(s1, HD // 2, 1)
        top = jnp.maximum(s0, s1)
        e0, e1 = jnp.exp2(s0 - top), jnp.exp2(s1 - top)
        return top, e0, e1, l0 * e0 + l1 * e1

    top, e0, e1, total = weights(stat_ref[core], d_stat[...])
    m_stat[...] = jnp.where(lane < HD // 2, top, pltpu.roll(total, HD // 2, 1))
    sy_copy = remote(m_stat, y_stat, st_send.at[1], st_recv.at[1], {'sp': cross})
    y_copies = []
    for i in range(blocks):
        d_copies[i].wait_recv()
        for r in range(span):
            b = i * span + r
            rows = pl.ds(b * group, group)
            m_acc[rows, :] = acc_ref[core, rows, :] * e0[:, b:b + 1] + d_acc[rows, :] * e1[:, b:b + 1]
        if i == 0:
            sy_copy.start()
        copy = remote(m_acc.at[pl.ds(i * height, height)], y_acc.at[pl.ds(i * height, height)],
                      y_send.at[i], y_recv.at[i], {'sp': cross})
        copy.start()
        y_copies.append(copy)
    sy_copy.wait_recv()
    top, e0, e1, total = weights(m_stat[...], y_stat[...])
    share = 1.0 / jnp.where(lane < HD // 2, total, 1.0)
    e0, e1 = e0 * share, e1 * share
    g_copies = []
    for i in range(blocks):
        y_copies[i].wait_recv()
        for r in range(span):
            b = i * span + r
            rows = pl.ds(b * group, group)
            val = m_acc[rows, :] * e0[:, b:b + 1] + y_acc[rows, :] * e1[:, b:b + 1]
            att[core, rows, :] = val.astype(BF16).astype(F32)
        copy = remote(att.at[core, pl.ds(i * height, height)], att.at[core, pl.ds(i * height, height)],
                      g_send.at[i], g_recv.at[i], {'sp': partner})
        copy.start()
        g_copies.append(copy)
    for i in range(blocks):
        g_copies[i].wait_recv()
    for g in range(2):
        for j in range(group):
            n = g * group + j
            a_ref[:, n * HD:(n + 1) * HD] = att[g, pl.ds(j, n_seq, stride=group), :].astype(BF16)
    w_copy.wait()

    chunks = part.shape[0]
    wide = 2 * CHUNK

    def compute(j):
        val = jnp.dot(a_ref[...], w_buf[:, j * wide:(j + 1) * wide], preferred_element_type=F32)
        part[2 * j] = val[:, :CHUNK]
        part[2 * j + 1] = val[:, CHUNK:]

    def emit(block, i, ref):
        at = pl.ds(pl.multiple_of(block * width + i * CHUNK, CHUNK), CHUNK)
        out_ref[:, at] = (h_ref[:, at].astype(F32) + ref[i]).astype(BF16)

    def e_copy(i):
        return remote(part.at[i], e_buf.at[i], e_send.at[i], e_recv.at[i], {'tp': hub_of_end})

    def b_copy(i):
        return remote(a_buf.at[i], b_buf.at[i], b_send.at[i], b_recv.at[i], {'tp': other_hub})

    def t_copy(i):
        return remote(tot.at[i], tot.at[i], t_send.at[i], t_recv.at[i], {'tp': end_of_hub})

    def y_copy(i):
        return remote(tot.at[i], y_buf.at[i], ys.at[i], yr.at[i], {'sp': cross})

    def p1_copy(i):
        return remote(tot.at[i], p1_buf.at[i], p1s.at[i], p1r.at[i], {'sp': partner})

    def p2_copy(i):
        return remote(y_buf.at[i], p2_buf.at[i], p2s.at[i], p2r.at[i], {'sp': partner})

    far = lax.rem(partner + 2, 4)

    def spread(i):
        y_copy(i).start()
        p1_copy(i).start()
        emit(sp, i, tot)

    def pass_on(i):
        y_copy(i).wait_recv()
        p2_copy(i).start()
        emit(cross, i, y_buf)

    @pl.when(is_hub)
    def _():
        lag, lag2 = 3, 6
        for j in range(chunks // 2):
            compute(j)
        for t in range(chunks + lag2):
            if t < chunks:
                e_copy(t).wait_recv()
                a_buf[t] = part[t] + e_buf[t]
                b_copy(t).start()
            i = t - lag
            if 0 <= i < chunks:
                b_copy(i).wait_recv()
                tot[i] = a_buf[i] + b_buf[i]
                t_copy(i).start()
                spread(i)
            i = t - lag2
            if 0 <= i < chunks:
                pass_on(i)
        for i in range(chunks):
            b_copy(i).wait_send()
            t_copy(i).wait_send()

    @pl.when(jnp.logical_not(is_hub))
    def _():
        lag = 3
        for j in range(chunks // 2):
            compute(j)
            e_copy(2 * j).start()
            e_copy(2 * j + 1).start()
        for t in range(chunks + lag):
            if t < chunks:
                t_copy(t).wait_recv()
                spread(t)
            i = t - lag
            if 0 <= i < chunks:
                pass_on(i)
        for i in range(chunks):
            e_copy(i).wait_send()

    for i in range(chunks):
        p1_copy(i).wait_recv()
        emit(partner, i, p1_buf)
        p2_copy(i).wait_recv()
        emit(far, i, p2_buf)
    for i in range(chunks):
        y_copy(i).wait_send()
        p1_copy(i).wait_send()
        p2_copy(i).wait_send()
    st_copy.wait_send()
    sy_copy.wait_send()
    for i in range(blocks):
        d_copies[i].wait_send()
        y_copies[i].wait_send()
        g_copies[i].wait_send()


def solution(mesh):
    cache_spec = P('dp', 'sp', 'tp', None)
    hbm = pl.BlockSpec(memory_space=pltpu.HBM)
    vmem = pl.BlockSpec(memory_space=pltpu.VMEM)
    smem = pl.BlockSpec(memory_space=pltpu.SMEM)
    dma = pltpu.SemaphoreType.DMA

    def local_step(hidden, norm_scale, w_qkv, w_out, k_cache, v_cache, positions):
        n_seq, seq_local, kv_local, head_dim = k_cache.shape
        d = hidden.shape[1]
        rows = seq_local * kv_local
        heads = w_qkv.shape[1] // head_dim
        group = heads // kv_local - 2
        k_flat = k_cache.reshape(n_seq, rows, head_dim)
        v_flat = v_cache.reshape(n_seq, rows, head_dim)
        cos_tab, sin_tab = rope_tables(positions)
        share = heads // 4
        cache_type = pltpu.VMEM((n_seq, rows, head_dim), BF16)
        qkv, k_vmem, v_vmem = pl.pallas_call(
            qkv_kernel,
            out_shape=[pltpu.VMEM((4, share, n_seq, head_dim), F32), cache_type, cache_type],
            in_specs=[vmem, vmem, vmem, vmem, hbm, hbm, hbm],
            out_specs=[vmem, vmem, vmem],
            scratch_shapes=[
                pltpu.VMEM((d, share * head_dim), BF16), pltpu.VMEM((n_seq, d), BF16),
                dma((8,)), dma((2,)), dma((3,)), dma((3,)),
            ],
            compiler_params=pltpu.CompilerParams(collective_id=0, has_side_effects=True, vmem_limit_bytes=24 << 20),
            name='qkv',
        )(hidden, norm_scale.reshape(1, d), cos_tab, sin_tab, *[pltpu.with_memory_space_constraint(a, pltpu.HBM) for a in (w_qkv, k_flat, v_flat)])
        qkv = qkv.reshape(heads, n_seq, head_dim)

        k_out, v_out, acc, stat = pl.pallas_call(
            attention_kernel,
            out_shape=[
                jax.ShapeDtypeStruct(k_flat.shape, BF16), jax.ShapeDtypeStruct(v_flat.shape, BF16),
                pltpu.VMEM((2, n_seq, group, head_dim), F32), pltpu.VMEM((2, group, head_dim), F32),
            ],
            in_specs=[smem, vmem, vmem, vmem],
            out_specs=[hbm, hbm, vmem, vmem],
            scratch_shapes=[pltpu.VMEM((n_seq * 2 * group, head_dim), F32), dma((2, 8))],
            compiler_params=pltpu.CompilerParams(vmem_limit_bytes=16 << 20),
            name='attention',
        )(positions, qkv, k_vmem, v_vmem)
        acc = acc.reshape(2, n_seq * group, head_dim)

        width = d // 4
        depth = w_out.shape[0]
        chunks = width // CHUNK
        blocks = 4
        slot = pltpu.VMEM((chunks, n_seq, CHUNK), F32)
        half = pltpu.VMEM((n_seq * group, head_dim), F32)
        tile = pltpu.VMEM((group, head_dim), F32)
        h_out = pl.pallas_call(
            project_kernel,
            out_shape=jax.ShapeDtypeStruct((n_seq, d), BF16),
            in_specs=[vmem, vmem, vmem, hbm],
            out_specs=vmem,
            scratch_shapes=[
                pltpu.VMEM((depth, width), BF16), half, tile, half, tile, half, tile,
                pltpu.VMEM((2, n_seq * group, head_dim), F32), pltpu.VMEM((n_seq, depth), BF16),
                slot, slot, slot, slot, slot, slot, slot, slot,
                dma(()), dma((2,)), dma((2,)), dma((blocks,)), dma((blocks,)), dma((blocks,)), dma((blocks,)),
                dma((blocks,)), dma((blocks,)),
                *[dma((chunks,)) for _ in range(12)],
            ],
            compiler_params=pltpu.CompilerParams(collective_id=1, has_side_effects=True, vmem_limit_bytes=40 << 20),
            name='project',
        )(hidden, acc, stat, pltpu.with_memory_space_constraint(w_out, pltpu.HBM))
        return h_out, k_out.reshape(k_cache.shape), v_out.reshape(v_cache.shape)

    return jax.shard_map(
        local_step,
        mesh=mesh,
        in_specs=(P('dp', None), P(None), P(None, 'tp'), P('tp', None), cache_spec, cache_spec, P('dp')),
        out_specs=(P('dp', None), cache_spec, cache_spec),
        check_vma=False,
    )
```

```python
import math
import jax
import jax.numpy as jnp
from jax import lax
from jax.experimental import pallas as pl
from jax.experimental.pallas import tpu as pltpu
from jax.sharding import PartitionSpec as P

F32 = jnp.float32
BF16 = jnp.bfloat16
HD = 128
NEG = -3e38
FLOOR = -1e38
MESH_ID = pl.DeviceIdType.MESH
CHUNK = 128


def remote(src, dst, send_sem, recv_sem, device_id):
    return pltpu.make_async_remote_copy(
        src_ref=src, dst_ref=dst, send_sem=send_sem, recv_sem=recv_sem, device_id=device_id, device_id_type=MESH_ID
    )


def sp_peers():
    sp = lax.axis_index('sp')
    return sp, sp + 1 - 2 * lax.rem(sp, 2), lax.rem(sp + 2, 4)


def enter(peers):
    barrier = pltpu.get_barrier_semaphore()
    for peer in peers:
        pl.semaphore_signal(barrier, inc=1, device_id=peer, device_id_type=MESH_ID)
    pl.semaphore_wait(barrier, len(peers))


def qkv_kernel(h_hbm, scale_hbm, pos_hbm, w_hbm, kc_hbm, vc_hbm, qkv_ref, k_ref, v_ref,
               h_ref, scale_ref, pos_ref, w0_buf, w1_buf, w2_buf, u_ref, cos_ref, sin_ref,
               i_sem, w_sem, c_sem, a_send, a_recv, b_send, b_recv, f_send, f_recv):
    sp, partner, cross = sp_peers()
    n_seq, d = h_ref.shape
    ins = [pltpu.make_async_copy(src, dst, i_sem.at[i])
           for i, (src, dst) in enumerate(((pos_hbm, pos_ref), (h_hbm, h_ref), (scale_hbm, scale_ref)))]
    for copy in ins:
        copy.start()
    bufs = (w0_buf, w1_buf, w2_buf)
    width = sum(buf.shape[1] for buf in bufs)
    pieces = w_sem.shape[1]
    depth = d // pieces
    w_copies, first = [], 0
    for g, buf in enumerate(bufs):
        col = pl.multiple_of(sp * width + first, HD)
        first += buf.shape[1]
        group = []
        for i in range(pieces):
            rows = pl.ds(i * depth, depth)
            copy = pltpu.make_async_copy(w_hbm.at[rows, pl.ds(col, buf.shape[1])], buf.at[rows], w_sem.at[g, i])
            copy.start()
            group.append(copy)
        w_copies.append(group)
    enter([{'sp': partner}, {'sp': cross}])

    ins[0].wait()
    row_id = lax.broadcasted_iota(jnp.int32, (n_seq, n_seq), 0)
    col_id = lax.broadcasted_iota(jnp.int32, (n_seq, n_seq), 1)
    pos = jnp.sum(jnp.where(row_id == col_id, pos_ref[...].astype(F32), 0.0), axis=-1, keepdims=True)
    lane = lax.broadcasted_iota(jnp.int32, (n_seq, HD), 1)
    freq = lax.rem(lane, HD // 2).astype(F32)
    angles = pos * jnp.exp(freq * (-2.0 * math.log(500000.0) / HD))
    cos_ref[...] = jnp.cos(angles)
    sin_part = jnp.sin(angles)
    sin_ref[...] = jnp.where(lane < HD // 2, -sin_part, sin_part)

    ins[1].wait()
    tiles = d // HD

    def tile(k):
        return h_ref[:, k * HD:(k + 1) * HD].astype(F32)

    total = tile(0)
    for k in range(1, tiles):
        total += tile(k)
    mean = jnp.sum(total, axis=-1, keepdims=True) * (1.0 / d)
    total = jnp.zeros((n_seq, HD), F32)
    for k in range(tiles):
        centered = tile(k) - mean
        total += centered * centered
    inv = lax.rsqrt(jnp.sum(total, axis=-1, keepdims=True) * (1.0 / d) + 1e-5)
    ins[2].wait()
    scale_rows = scale_ref[...].astype(F32)
    for k in range(tiles):
        u_ref[:, k * HD:(k + 1) * HD] = ((tile(k) - mean) * inv * scale_rows[k:k + 1, :]).astype(BF16)

    cache_copies = [pltpu.make_async_copy(kc_hbm, k_ref, c_sem.at[0]), pltpu.make_async_copy(vc_hbm, v_ref, c_sem.at[1])]
    odd = lax.rem(sp, 2)
    heads = width // HD
    to_cross, to_partner, forward = [], [], []
    j = 0
    for g, buf in enumerate(bufs):
        acc = None
        for i in range(pieces):
            w_copies[g][i].wait()
            rows = slice(i * depth, (i + 1) * depth)
            part = jnp.dot(u_ref[:, rows], buf[rows, :], preferred_element_type=F32)
            acc = part if acc is None else acc + part
        if g >= 1:
            cache_copies[g - 1].start()
        proj = jnp.clip(acc.astype(BF16).astype(F32), -8.0, 8.0)
        n = buf.shape[1] // HD
        for r in range(n):
            val = proj[:, r * HD:(r + 1) * HD]
            rot = (val * cos_ref[...] + pltpu.roll(val, HD // 2, 1) * sin_ref[...]).astype(BF16).astype(F32)
            if j + r == heads - 1:
                rot = jnp.where(odd == 1, val, rot)
            qkv_ref[sp, j + r] = rot
        mine = qkv_ref.at[sp, pl.ds(j, n)]
        theirs = qkv_ref.at[cross, pl.ds(j, n)]
        to_cross.append(remote(mine, mine, a_send.at[g], a_recv.at[g], {'sp': cross}))
        to_partner.append(remote(mine, mine, b_send.at[g], b_recv.at[g], {'sp': partner}))
        forward.append(remote(theirs, theirs, f_send.at[g], f_recv.at[g], {'sp': partner}))
        to_cross[g].start()
        to_partner[g].start()
        j += n
    for g in range(len(bufs)):
        to_cross[g].wait_recv()
        forward[g].start()
    for copy in cache_copies:
        copy.wait()
    for g in range(len(bufs)):
        to_partner[g].wait()
        to_cross[g].wait_send()
        forward[g].wait()


def attention_kernel(pos_ref, qkv_ref, k_ref, v_ref, k_out, v_out, acc_ref, stat_ref, q_ref, s_ref, p_ref, out_sem):
    n_seq, rows, _ = k_ref.shape
    seq_local = rows // 2
    group = acc_ref.shape[2]
    base = lax.axis_index('sp') * seq_local
    per_kv = group + 2
    n_q = 2 * group

    tile = 16
    row_id = lax.broadcasted_iota(jnp.int32, (tile, HD), 0)
    at_once = 8

    def patch(i, carry):
        for r in range(at_once):
            b = i * at_once + r
            row = 2 * (pos_ref[b] - base)
            start = pl.multiple_of(jnp.clip(row // tile, 0, rows // tile - 1) * tile, tile)
            off = row - start
            for ref, slot in ((k_ref, group), (v_ref, group + 1)):
                block = ref[b, pl.ds(start, tile), :].astype(F32)
                one = qkv_ref[slot, pl.ds(b, 1), :]
                two = qkv_ref[per_kv + slot, pl.ds(b, 1), :]
                block = jnp.where(row_id == off, one, jnp.where(row_id == off + 1, two, block))
                ref[b, pl.ds(start, tile), :] = block.astype(BF16)
        return carry

    lax.fori_loop(0, n_seq // at_once, patch, 0)
    pieces = out_sem.shape[1]
    span = n_seq // pieces
    copies = []
    for i in range(pieces):
        for s, (src, dst) in enumerate(((k_ref, k_out), (v_ref, v_out))):
            copy = pltpu.make_async_copy(src.at[pl.ds(i * span, span)], dst.at[pl.ds(i * span, span)], out_sem.at[s, i])
            copy.start()
            copies.append(copy)
    for g in range(2):
        for j in range(group):
            q_ref[pl.ds(g * group + j, n_seq, stride=n_q), :] = qkv_ref[g * per_kv + j]

    col_id = lax.broadcasted_iota(jnp.int32, (n_q, rows), 1)
    head_id = lax.broadcasted_iota(jnp.int32, (n_q, rows), 0) // group
    col_key = jnp.where(lax.rem(col_id, 2) == head_id, col_id, 1 << 30)
    lane = lax.broadcasted_iota(jnp.int32, (n_q, HD), 1)
    upper = lax.broadcasted_iota(jnp.int32, (2 * n_q, HD), 0) < n_q
    factor = HD ** -0.5 * math.log2(math.e)
    pairs = s_ref.shape[0] // (2 * n_q)
    batch = 2 * pairs

    def score(i):
        for r in range(pairs):
            b = i * batch + 2 * r
            q = q_ref[pl.ds(pl.multiple_of(b * n_q, 2 * n_q), 2 * n_q), :]
            lhs = jnp.concatenate([jnp.where(upper, q, 0.0), jnp.where(upper, 0.0, q)], axis=1).astype(BF16)
            rhs = jnp.concatenate([k_ref[b], k_ref[b + 1]], axis=1)
            out = lax.dot_general(lhs, rhs, (((1,), (1,)), ((), ())), preferred_element_type=F32)
            for e in range(2):
                limit = 2 * (pos_ref[b + e] - base + 1)
                half = out[e * n_q:(e + 1) * n_q] * factor
                s_ref[(2 * r + e) * n_q:(2 * r + e + 1) * n_q, :] = jnp.where(col_key < limit, half, NEG)

    def soften(i, stats):
        for r in range(batch):
            b = i * batch + r
            scores = s_ref[r * n_q:(r + 1) * n_q, :]
            top = jnp.maximum(jnp.max(scores, axis=-1, keepdims=True), FLOOR)
            probs = jnp.exp2(scores - top)
            total = jnp.sum(probs, axis=-1, keepdims=True)
            p_ref[r * n_q:(r + 1) * n_q, :] = probs.astype(BF16)
            stats = jnp.where(lane == b, top, jnp.where(lane == b + n_seq, total, stats))
        return stats

    def weigh(i):
        for r in range(pairs):
            b = i * batch + 2 * r
            rhs = jnp.concatenate([v_ref[b], v_ref[b + 1]], axis=1)
            out = jnp.dot(p_ref[2 * r * n_q:(2 * r + 2) * n_q, :], rhs, preferred_element_type=F32)
            for e in range(2):
                own = out[e * n_q:(e + 1) * n_q, e * HD:(e + 1) * HD]
                acc_ref[0, b + e] = own[:group]
                acc_ref[1, b + e] = own[group:]

    steps = n_seq // batch
    stats = jnp.zeros((n_q, HD), F32)
    score(0)
    stats = soften(0, stats)
    score(1)

    def step(i, stats):
        weigh(i)
        stats = soften(i + 1, stats)
        score(i + 2)
        return stats

    stats = lax.fori_loop(0, steps - 2, step, stats)
    weigh(steps - 2)
    stats = soften(steps - 1, stats)
    weigh(steps - 1)
    stat_ref[0] = stats[:group]
    stat_ref[1] = stats[group:]
    for copy in copies:
        copy.wait()


def project_kernel(h_ref, acc_ref, stat_ref, w_hbm, out_ref, w_buf, d_acc, d_stat, m_acc, m_stat, y_acc, y_stat, att, a_ref,
                   part, e_buf, a_buf, b_buf, tot, y_buf, p1_buf, p2_buf,
                   w_sem, st_send, st_recv, d_send, d_recv, y_send, y_recv, g_send, g_recv,
                   e_send, e_recv, b_send, b_recv, t_send, t_recv, ys, yr, p1s, p1r, p2s, p2r):
    sp, partner, cross = sp_peers()
    core = lax.rem(sp, 2)
    y = sp // 2
    z = lax.axis_index('tp')
    is_hub = (z == 1) | (z == 2)
    end_of_hub = 3 * (z - 1)
    hub_of_end = 1 + z // 2
    other_hub = 3 - z
    width = w_buf.shape[1]
    col = pl.multiple_of(core * width, HD)
    w_copy = pltpu.make_async_copy(w_hbm.at[:, pl.ds(col, width)], w_buf, w_sem)
    w_copy.start()

    barrier = pltpu.get_barrier_semaphore()
    for peer in ({'sp': partner}, {'sp': cross}):
        pl.semaphore_signal(barrier, inc=1, device_id=peer, device_id_type=MESH_ID)

    @pl.when(is_hub)
    def _():
        for peer in ({'tp': end_of_hub}, {'tp': other_hub}):
            pl.semaphore_signal(barrier, inc=1, device_id=peer, device_id_type=MESH_ID)
        pl.semaphore_wait(barrier, 4)

    @pl.when(jnp.logical_not(is_hub))
    def _():
        pl.semaphore_signal(barrier, inc=1, device_id={'tp': hub_of_end}, device_id_type=MESH_ID)
        pl.semaphore_wait(barrier, 3)

    group = stat_ref.shape[1]
    seqs = out_ref.shape[0] // 2
    blocks = y_send.shape[0]
    span = seqs // blocks
    height = span * group
    other = 1 - core
    st_copy = remote(stat_ref.at[other], d_stat, st_send.at[0], st_recv.at[0], {'sp': partner})
    st_copy.start()

    def rows_of(half, i):
        return pl.ds(pl.multiple_of((half * blocks + i) * height, height), height)

    d_copies = []
    for n in range(2 * blocks):
        rows = rows_of(1 - y if n < blocks else y, n % blocks)
        copy = remote(acc_ref.at[other, rows], d_acc.at[rows], d_send.at[n], d_recv.at[n], {'sp': partner})
        copy.start()
        d_copies.append(copy)
    st_copy.wait_recv()
    lane = lax.broadcasted_iota(jnp.int32, (group, HD), 1)

    def weights(s0, s1):
        l0, l1 = pltpu.roll(s0, HD // 2, 1), pltpu.roll(s1, HD // 2, 1)
        top = jnp.maximum(s0, s1)
        e0, e1 = jnp.exp2(s0 - top), jnp.exp2(s1 - top)
        return top, e0, e1, l0 * e0 + l1 * e1

    def lanes_of(half, val):
        return jnp.where(half == 0, val, pltpu.roll(val, HD - seqs, 1))

    top, e0, e1, total = weights(stat_ref[core], d_stat[...])
    m_stat[...] = jnp.where(lane < HD // 2, top, pltpu.roll(total, HD // 2, 1))
    sy_copy = remote(m_stat, y_stat, st_send.at[1], st_recv.at[1], {'sp': cross})
    y_copies = []
    for n in range(2 * blocks):
        half, i = (1 - y if n < blocks else y), n % blocks
        d_copies[n].wait_recv()
        f0, f1 = lanes_of(half, e0), lanes_of(half, e1)
        first = half * seqs * group
        for r in range(span):
            b = i * span + r
            rows = pl.ds(pl.multiple_of(first + b * group, group), group)
            m_acc[rows, :] = acc_ref[core, rows, :] * f0[:, b:b + 1] + d_acc[rows, :] * f1[:, b:b + 1]
        if n == 0:
            sy_copy.start()
        if n < blocks:
            copy = remote(m_acc.at[rows_of(half, i)], y_acc.at[pl.ds(i * height, height)], y_send.at[i], y_recv.at[i], {'sp': cross})
            copy.start()
            y_copies.append(copy)
    sy_copy.wait_recv()
    top, e0, e1, total = weights(m_stat[...], y_stat[...])
    share = 1.0 / jnp.where(lane < HD // 2, total, 1.0)
    e0, e1 = lanes_of(y, e0 * share), lanes_of(y, e1 * share)
    first = y * seqs * group
    g_copies = []
    for i in range(blocks):
        y_copies[i].wait_recv()
        for r in range(span):
            b = i * span + r
            rows = pl.ds(b * group, group)
            mine = m_acc[pl.ds(pl.multiple_of(first + b * group, group), group), :]
            val = mine * e0[:, b:b + 1] + y_acc[rows, :] * e1[:, b:b + 1]
            att[core, rows, :] = val.astype(BF16).astype(F32)
        block = att.at[core, pl.ds(i * height, height)]
        copy = remote(block, block, g_send.at[i], g_recv.at[i], {'sp': partner})
        copy.start()
        g_copies.append(copy)
    for i in range(blocks):
        g_copies[i].wait_recv()
    for g in range(2):
        for j in range(group):
            n = g * group + j
            a_ref[:, n * HD:(n + 1) * HD] = att[g, pl.ds(j, seqs, stride=group), :].astype(BF16)
    w_copy.wait()

    chunks = part.shape[0]
    wide = part.shape[2]

    def compute(j):
        part[j] = jnp.dot(a_ref[...], w_buf[:, j * wide:(j + 1) * wide], preferred_element_type=F32)

    def emit(half, side, i, ref):
        at = (pl.ds(pl.multiple_of(half * seqs, seqs), seqs), pl.ds(pl.multiple_of(side * width + i * wide, wide), wide))
        out_ref[at] = (h_ref[at].astype(F32) + ref[i]).astype(BF16)

    def e_copy(i):
        return remote(part.at[i], e_buf.at[i], e_send.at[i], e_recv.at[i], {'tp': hub_of_end})

    def b_copy(i):
        return remote(a_buf.at[i], b_buf.at[i], b_send.at[i], b_recv.at[i], {'tp': other_hub})

    def t_copy(i):
        return remote(tot.at[i], tot.at[i], t_send.at[i], t_recv.at[i], {'tp': end_of_hub})

    def y_copy(i):
        return remote(tot.at[i], y_buf.at[i], ys.at[i], yr.at[i], {'sp': cross})

    def p1_copy(i):
        return remote(tot.at[i], p1_buf.at[i], p1s.at[i], p1r.at[i], {'sp': partner})

    def p2_copy(i):
        return remote(y_buf.at[i], p2_buf.at[i], p2s.at[i], p2r.at[i], {'sp': partner})

    def spread(i):
        y_copy(i).start()
        p1_copy(i).start()
        emit(y, core, i, tot)

    def pass_on(i):
        y_copy(i).wait_recv()
        p2_copy(i).start()
        emit(1 - y, core, i, y_buf)

    @pl.when(is_hub)
    def _():
        lag, lag2 = 3, 7
        for j in range(chunks):
            compute(j)
        for t in range(chunks + lag2):
            if t < chunks:
                e_copy(t).wait_recv()
                a_buf[t] = part[t] + e_buf[t]
                b_copy(t).start()
            i = t - lag
            if 0 <= i < chunks:
                b_copy(i).wait_recv()
                tot[i] = a_buf[i] + b_buf[i]
                t_copy(i).start()
                spread(i)
            i = t - lag2
            if 0 <= i < chunks:
                pass_on(i)
        for i in range(chunks):
            b_copy(i).wait_send()
            t_copy(i).wait_send()

    @pl.when(jnp.logical_not(is_hub))
    def _():
        lag = 4
        for j in range(chunks):
            compute(j)
            if j > 0:
                e_copy(j - 1).start()
        e_copy(chunks - 1).start()
        for t in range(chunks + lag):
            if t < chunks:
                t_copy(t).wait_recv()
                spread(t)
            i = t - lag
            if 0 <= i < chunks:
                pass_on(i)
        for i in range(chunks):
            e_copy(i).wait_send()

    for i in range(chunks):
        p1_copy(i).wait_recv()
        emit(y, other, i, p1_buf)
        p2_copy(i).wait_recv()
        emit(1 - y, other, i, p2_buf)
    for i in range(chunks):
        y_copy(i).wait_send()
        p1_copy(i).wait_send()
        p2_copy(i).wait_send()
    st_copy.wait_send()
    sy_copy.wait_send()
    for copy in d_copies + y_copies + g_copies:
        copy.wait_send()


def solution(mesh):
    cache_spec = P('dp', 'sp', 'tp', None)
    hbm = pl.BlockSpec(memory_space=pltpu.HBM)
    vmem = pl.BlockSpec(memory_space=pltpu.VMEM)
    smem = pl.BlockSpec(memory_space=pltpu.SMEM)
    dma = pltpu.SemaphoreType.DMA

    def local_step(hidden, norm_scale, w_qkv, w_out, k_cache, v_cache, positions):
        n_seq, seq_local, kv_local, head_dim = k_cache.shape
        d = hidden.shape[1]
        rows = seq_local * kv_local
        heads = w_qkv.shape[1] // head_dim
        group = heads // kv_local - 2
        k_flat = k_cache.reshape(n_seq, rows, head_dim)
        v_flat = v_cache.reshape(n_seq, rows, head_dim)
        share = heads // 4
        in_hbm = [pltpu.with_memory_space_constraint(a, pltpu.HBM)
                  for a in (hidden, norm_scale.reshape(d // head_dim, head_dim), positions.reshape(1, n_seq), w_qkv, k_flat, v_flat)]
        cache_type = pltpu.VMEM((n_seq, rows, head_dim), BF16)
        table = pltpu.VMEM((n_seq, head_dim), F32)
        groups = [2, 2, share - 4]
        qkv, k_vmem, v_vmem = pl.pallas_call(
            qkv_kernel,
            out_shape=[pltpu.VMEM((4, share, n_seq, head_dim), F32), cache_type, cache_type],
            in_specs=[hbm] * 6,
            out_specs=[vmem, vmem, vmem],
            scratch_shapes=[
                pltpu.VMEM((n_seq, d), BF16), pltpu.VMEM((d // head_dim, head_dim), BF16), pltpu.VMEM((1, n_seq), jnp.int32),
                *[pltpu.VMEM((d, n * head_dim), BF16) for n in groups], pltpu.VMEM((n_seq, d), BF16), table, table,
                dma((3,)), dma((3, 2)), dma((2,)), *[dma((3,)) for _ in range(6)],
            ],
            compiler_params=pltpu.CompilerParams(collective_id=0, has_side_effects=True, vmem_limit_bytes=24 << 20),
            name='qkv',
        )(*in_hbm)
        qkv = qkv.reshape(heads, n_seq, head_dim)

        batch = 8
        k_out, v_out, acc, stat = pl.pallas_call(
            attention_kernel,
            out_shape=[
                jax.ShapeDtypeStruct(k_flat.shape, BF16), jax.ShapeDtypeStruct(v_flat.shape, BF16),
                pltpu.VMEM((2, n_seq, group, head_dim), F32), pltpu.VMEM((2, group, head_dim), F32),
            ],
            in_specs=[smem, vmem, vmem, vmem],
            out_specs=[hbm, hbm, vmem, vmem],
            scratch_shapes=[
                pltpu.VMEM((n_seq * 2 * group, head_dim), F32), pltpu.VMEM((batch * 2 * group, rows), F32),
                pltpu.VMEM((batch * 2 * group, rows), BF16), dma((2, 8)),
            ],
            compiler_params=pltpu.CompilerParams(vmem_limit_bytes=16 << 20),
            name='attention',
        )(positions, qkv, k_vmem, v_vmem)
        acc = acc.reshape(2, n_seq * group, head_dim)

        width = d // 2
        depth = w_out.shape[0]
        wide = 2 * CHUNK
        chunks = width // wide
        blocks = 2
        seqs = n_seq // 2
        slot = pltpu.VMEM((chunks, seqs, wide), F32)
        whole = pltpu.VMEM((n_seq * group, head_dim), F32)
        half = pltpu.VMEM((seqs * group, head_dim), F32)
        tile = pltpu.VMEM((group, head_dim), F32)
        h_out = pl.pallas_call(
            project_kernel,
            out_shape=jax.ShapeDtypeStruct((n_seq, d), BF16),
            in_specs=[vmem, vmem, vmem, hbm],
            out_specs=vmem,
            scratch_shapes=[
                pltpu.VMEM((depth, width), BF16), whole, tile, whole, tile, half, tile,
                pltpu.VMEM((2, seqs * group, head_dim), F32), pltpu.VMEM((seqs, depth), BF16),
                slot, slot, slot, slot, slot, slot, slot, slot,
                dma(()), dma((2,)), dma((2,)), dma((2 * blocks,)), dma((2 * blocks,)), *[dma((blocks,)) for _ in range(4)],
                *[dma((chunks,)) for _ in range(12)],
            ],
            compiler_params=pltpu.CompilerParams(collective_id=1, has_side_effects=True, vmem_limit_bytes=40 << 20),
            name='project',
        )(hidden, acc, stat, pltpu.with_memory_space_constraint(w_out, pltpu.HBM))
        return h_out, k_out.reshape(k_cache.shape), v_out.reshape(v_cache.shape)

    return jax.shard_map(
        local_step,
        mesh=mesh,
        in_specs=(P('dp', None), P(None), P(None, 'tp'), P('tp', None), cache_spec, cache_spec, P('dp')),
        out_specs=(P('dp', None), cache_spec, cache_spec),
        check_vma=False,
    )
```

```python
import math
import jax
import jax.numpy as jnp
from jax import lax
from jax.experimental import pallas as pl
from jax.experimental.pallas import tpu as pltpu
from jax.sharding import PartitionSpec as P

F32 = jnp.float32
BF16 = jnp.bfloat16
HD = 128
NEG = -3e38
FLOOR = -1e38
MESH_ID = pl.DeviceIdType.MESH
CHUNK = 128


def remote(src, dst, send_sem, recv_sem, device_id):
    return pltpu.make_async_remote_copy(
        src_ref=src, dst_ref=dst, send_sem=send_sem, recv_sem=recv_sem, device_id=device_id, device_id_type=MESH_ID
    )


def sp_peers():
    sp = lax.axis_index('sp')
    return sp, sp + 1 - 2 * lax.rem(sp, 2), lax.rem(sp + 2, 4)


def enter(peers):
    barrier = pltpu.get_barrier_semaphore()
    for peer in peers:
        pl.semaphore_signal(barrier, inc=1, device_id=peer, device_id_type=MESH_ID)
    pl.semaphore_wait(barrier, len(peers))


def qkv_kernel(h_hbm, scale_hbm, pos_hbm, w_hbm, kc_hbm, vc_hbm, qkv_ref, k_ref, v_ref,
               h_ref, scale_ref, pos_ref, w0_buf, w1_buf, w2_buf, u_ref, cos_ref, sin_ref,
               i_sem, w_sem, c_sem, a_send, a_recv, b_send, b_recv, f_send, f_recv):
    sp, partner, cross = sp_peers()
    n_seq, d = h_ref.shape
    ins = [pltpu.make_async_copy(src, dst, i_sem.at[i])
           for i, (src, dst) in enumerate(((pos_hbm, pos_ref), (h_hbm, h_ref), (scale_hbm, scale_ref)))]
    for copy in ins:
        copy.start()
    bufs = (w0_buf, w1_buf, w2_buf)
    width = sum(buf.shape[1] for buf in bufs)
    pieces = w_sem.shape[1]
    depth = d // pieces
    w_copies, first = [], 0
    for g, buf in enumerate(bufs):
        col = pl.multiple_of(sp * width + first, HD)
        first += buf.shape[1]

        def w_copy(i, g=g, buf=buf, col=col):
            rows = pl.ds(pl.multiple_of(i * depth, depth), depth)
            return pltpu.make_async_copy(w_hbm.at[rows, pl.ds(col, buf.shape[1])], buf.at[rows], w_sem.at[g, i])

        lax.fori_loop(0, pieces, lambda i, carry, w_copy=w_copy: (w_copy(i).start(), carry)[1], 0)
        w_copies.append([w_copy(i) for i in range(pieces)])
    enter([{'sp': partner}, {'sp': cross}])

    ins[0].wait()
    row_id = lax.broadcasted_iota(jnp.int32, (n_seq, n_seq), 0)
    col_id = lax.broadcasted_iota(jnp.int32, (n_seq, n_seq), 1)
    pos = jnp.sum(jnp.where(row_id == col_id, pos_ref[...].astype(F32), 0.0), axis=-1, keepdims=True)
    lane = lax.broadcasted_iota(jnp.int32, (n_seq, HD), 1)
    freq = lax.rem(lane, HD // 2).astype(F32)
    angles = pos * jnp.exp(freq * (-2.0 * math.log(500000.0) / HD))
    cos_ref[...] = jnp.cos(angles)
    sin_part = jnp.sin(angles)
    sin_ref[...] = jnp.where(lane < HD // 2, -sin_part, sin_part)

    ins[1].wait()
    tiles = d // HD

    def tile(k):
        return h_ref[:, k * HD:(k + 1) * HD].astype(F32)

    total = tile(0)
    for k in range(1, tiles):
        total += tile(k)
    mean = jnp.sum(total, axis=-1, keepdims=True) * (1.0 / d)
    total = jnp.zeros((n_seq, HD), F32)
    for k in range(tiles):
        centered = tile(k) - mean
        total += centered * centered
    inv = lax.rsqrt(jnp.sum(total, axis=-1, keepdims=True) * (1.0 / d) + 1e-5)
    ins[2].wait()
    scale_rows = scale_ref[...].astype(F32)
    for k in range(tiles):
        u_ref[:, k * HD:(k + 1) * HD] = ((tile(k) - mean) * inv * scale_rows[k:k + 1, :]).astype(BF16)

    cache_copies = [pltpu.make_async_copy(kc_hbm, k_ref, c_sem.at[0]), pltpu.make_async_copy(vc_hbm, v_ref, c_sem.at[1])]
    odd = lax.rem(sp, 2)
    heads = width // HD
    to_cross, to_partner, forward = [], [], []
    j = 0
    for g, buf in enumerate(bufs):
        acc = None
        for i in range(pieces):
            w_copies[g][i].wait()
            rows = slice(i * depth, (i + 1) * depth)
            if g >= 1 and i == 0:
                cache_copies[g - 1].start()
            part = jnp.dot(u_ref[:, rows], buf[rows, :], preferred_element_type=F32)
            acc = part if acc is None else acc + part
        proj = jnp.clip(acc.astype(BF16).astype(F32), -8.0, 8.0)
        n = buf.shape[1] // HD
        for r in range(n):
            val = proj[:, r * HD:(r + 1) * HD]
            rot = (val * cos_ref[...] + pltpu.roll(val, HD // 2, 1) * sin_ref[...]).astype(BF16).astype(F32)
            if j + r == heads - 1:
                rot = jnp.where(odd == 1, val, rot)
            qkv_ref[sp, j + r] = rot
        mine = qkv_ref.at[sp, pl.ds(j, n)]
        theirs = qkv_ref.at[cross, pl.ds(j, n)]
        to_cross.append(remote(mine, mine, a_send.at[g], a_recv.at[g], {'sp': cross}))
        to_partner.append(remote(mine, mine, b_send.at[g], b_recv.at[g], {'sp': partner}))
        forward.append(remote(theirs, theirs, f_send.at[g], f_recv.at[g], {'sp': partner}))
        to_cross[g].start()
        to_partner[g].start()
        j += n
    for g in range(len(bufs)):
        to_cross[g].wait_recv()
        forward[g].start()
    for copy in cache_copies:
        copy.wait()
    for g in range(len(bufs)):
        to_partner[g].wait()
        to_cross[g].wait_send()
        forward[g].wait()


def attention_kernel(pos_ref, qkv_ref, k_ref, v_ref, k_out, v_out, acc_ref, stat_ref, q_ref, s_ref, p_ref, out_sem):
    n_seq, rows, _ = k_ref.shape
    seq_local = rows // 2
    group = acc_ref.shape[2]
    base = lax.axis_index('sp') * seq_local
    per_kv = group + 2
    n_q = 2 * group

    tile = 16
    row_id = lax.broadcasted_iota(jnp.int32, (tile, HD), 0)
    at_once = 8

    def patch(i, carry):
        for r in range(at_once):
            b = i * at_once + r
            row = 2 * (pos_ref[b] - base)
            start = pl.multiple_of(jnp.clip(row // tile, 0, rows // tile - 1) * tile, tile)
            off = row - start
            for ref, slot in ((k_ref, group), (v_ref, group + 1)):
                block = ref[b, pl.ds(start, tile), :].astype(F32)
                one = qkv_ref[slot, pl.ds(b, 1), :]
                two = qkv_ref[per_kv + slot, pl.ds(b, 1), :]
                block = jnp.where(row_id == off, one, jnp.where(row_id == off + 1, two, block))
                ref[b, pl.ds(start, tile), :] = block.astype(BF16)
        return carry

    def out_copies(i):
        span = pl.ds(i * at_once, at_once)
        return [pltpu.make_async_copy(src.at[span], dst.at[span], out_sem.at[n, i])
                for n, (src, dst) in enumerate(((k_ref, k_out), (v_ref, v_out)))]

    def patch_and_write(i, carry):
        patch(i, carry)
        for copy in out_copies(i - 1):
            copy.start()
        return carry

    pieces = n_seq // at_once
    patch(0, 0)
    lax.fori_loop(1, pieces, patch_and_write, 0)
    for g in range(2):
        for j in range(group):
            q_ref[pl.ds(g * group + j, n_seq, stride=n_q), :] = qkv_ref[g * per_kv + j]
    for copy in out_copies(pieces - 1):
        copy.start()

    col_id = lax.broadcasted_iota(jnp.int32, (n_q, rows), 1)
    head_id = lax.broadcasted_iota(jnp.int32, (n_q, rows), 0) // group
    col_key = jnp.where(lax.rem(col_id, 2) == head_id, col_id, 1 << 30)
    lane = lax.broadcasted_iota(jnp.int32, (n_q, HD), 1)
    upper = lax.broadcasted_iota(jnp.int32, (2 * n_q, HD), 0) < n_q
    factor = HD ** -0.5 * math.log2(math.e)
    pairs = s_ref.shape[0] // (2 * n_q)
    batch = 2 * pairs

    def score(i):
        for r in range(pairs):
            b = i * batch + 2 * r
            q = q_ref[pl.ds(pl.multiple_of(b * n_q, 2 * n_q), 2 * n_q), :]
            lhs = jnp.concatenate([jnp.where(upper, q, 0.0), jnp.where(upper, 0.0, q)], axis=1).astype(BF16)
            rhs = jnp.concatenate([k_ref[b], k_ref[b + 1]], axis=1)
            out = lax.dot_general(lhs, rhs, (((1,), (1,)), ((), ())), preferred_element_type=F32)
            for e in range(2):
                limit = 2 * (pos_ref[b + e] - base + 1)
                half = out[e * n_q:(e + 1) * n_q] * factor
                s_ref[(2 * r + e) * n_q:(2 * r + e + 1) * n_q, :] = jnp.where(col_key < limit, half, NEG)

    def soften(i, stats):
        for r in range(batch):
            b = i * batch + r
            scores = s_ref[r * n_q:(r + 1) * n_q, :]
            top = jnp.maximum(jnp.max(scores, axis=-1, keepdims=True), FLOOR)
            probs = jnp.exp2(scores - top)
            total = jnp.sum(probs, axis=-1, keepdims=True)
            p_ref[r * n_q:(r + 1) * n_q, :] = probs.astype(BF16)
            stats = jnp.where(lane == b, top, jnp.where(lane == b + n_seq, total, stats))
        return stats

    def weigh(i):
        for r in range(pairs):
            b = i * batch + 2 * r
            rhs = jnp.concatenate([v_ref[b], v_ref[b + 1]], axis=1)
            out = jnp.dot(p_ref[2 * r * n_q:(2 * r + 2) * n_q, :], rhs, preferred_element_type=F32)
            for e in range(2):
                own = out[e * n_q:(e + 1) * n_q, e * HD:(e + 1) * HD]
                acc_ref[0, b + e] = own[:group]
                acc_ref[1, b + e] = own[group:]

    steps = n_seq // batch
    stats = jnp.zeros((n_q, HD), F32)
    score(0)
    stats = soften(0, stats)
    score(1)

    def step(i, stats):
        weigh(i)
        stats = soften(i + 1, stats)
        score(i + 2)
        return stats

    stats = lax.fori_loop(0, steps - 2, step, stats)
    weigh(steps - 2)
    stats = soften(steps - 1, stats)
    weigh(steps - 1)
    stat_ref[0] = stats[:group]
    stat_ref[1] = stats[group:]
    for i in range(pieces):
        for copy in out_copies(i):
            copy.wait()


def project_kernel(h_ref, acc_ref, stat_ref, w_hbm, out_ref, w_buf, d_acc, d_stat, m_acc, m_stat, y_acc, y_stat, att, a_ref,
                   part, e_buf, a_buf, b_buf, tot, y_buf, p1_buf, p2_buf,
                   w_sem, st_send, st_recv, d_send, d_recv, y_send, y_recv, g_send, g_recv,
                   e_send, e_recv, b_send, b_recv, t_send, t_recv, ys, yr, p1s, p1r, p2s, p2r):
    sp, partner, cross = sp_peers()
    core = lax.rem(sp, 2)
    y = sp // 2
    z = lax.axis_index('tp')
    is_hub = (z == 1) | (z == 2)
    end_of_hub = 3 * (z - 1)
    hub_of_end = 1 + z // 2
    other_hub = 3 - z
    width = w_buf.shape[1]
    col = pl.multiple_of(core * width, HD)
    w_copy = pltpu.make_async_copy(w_hbm.at[:, pl.ds(col, width)], w_buf, w_sem)
    w_copy.start()

    barrier = pltpu.get_barrier_semaphore()
    for peer in ({'sp': partner}, {'sp': cross}):
        pl.semaphore_signal(barrier, inc=1, device_id=peer, device_id_type=MESH_ID)

    @pl.when(is_hub)
    def _():
        for peer in ({'tp': end_of_hub}, {'tp': other_hub}):
            pl.semaphore_signal(barrier, inc=1, device_id=peer, device_id_type=MESH_ID)
        pl.semaphore_wait(barrier, 4)

    @pl.when(jnp.logical_not(is_hub))
    def _():
        pl.semaphore_signal(barrier, inc=1, device_id={'tp': hub_of_end}, device_id_type=MESH_ID)
        pl.semaphore_wait(barrier, 3)

    group = stat_ref.shape[1]
    seqs = out_ref.shape[0] // 2
    blocks = y_send.shape[0]
    span = seqs // blocks
    height = span * group
    other = 1 - core
    st_copy = remote(stat_ref.at[other], d_stat, st_send.at[0], st_recv.at[0], {'sp': partner})
    st_copy.start()

    def rows_of(half, i):
        return pl.ds(pl.multiple_of((half * blocks + i) * height, height), height)

    d_copies = []
    for n in range(2 * blocks):
        rows = rows_of(1 - y if n < blocks else y, n % blocks)
        copy = remote(acc_ref.at[other, rows], d_acc.at[rows], d_send.at[n], d_recv.at[n], {'sp': partner})
        copy.start()
        d_copies.append(copy)
    st_copy.wait_recv()
    lane = lax.broadcasted_iota(jnp.int32, (group, HD), 1)

    def weights(s0, s1):
        l0, l1 = pltpu.roll(s0, HD // 2, 1), pltpu.roll(s1, HD // 2, 1)
        top = jnp.maximum(s0, s1)
        e0, e1 = jnp.exp2(s0 - top), jnp.exp2(s1 - top)
        return top, e0, e1, l0 * e0 + l1 * e1

    def lanes_of(half, val):
        return jnp.where(half == 0, val, pltpu.roll(val, HD - seqs, 1))

    top, e0, e1, total = weights(stat_ref[core], d_stat[...])
    m_stat[...] = jnp.where(lane < HD // 2, top, pltpu.roll(total, HD // 2, 1))
    sy_copy = remote(m_stat, y_stat, st_send.at[1], st_recv.at[1], {'sp': cross})
    y_copies = []
    for n in range(2 * blocks):
        half, i = (1 - y if n < blocks else y), n % blocks
        d_copies[n].wait_recv()
        f0, f1 = lanes_of(half, e0), lanes_of(half, e1)
        first = half * seqs * group
        for r in range(span):
            b = i * span + r
            rows = pl.ds(pl.multiple_of(first + b * group, group), group)
            m_acc[rows, :] = acc_ref[core, rows, :] * f0[:, b:b + 1] + d_acc[rows, :] * f1[:, b:b + 1]
        if n == 0:
            sy_copy.start()
        if n < blocks:
            copy = remote(m_acc.at[rows_of(half, i)], y_acc.at[pl.ds(i * height, height)], y_send.at[i], y_recv.at[i], {'sp': cross})
            copy.start()
            y_copies.append(copy)
    sy_copy.wait_recv()
    top, e0, e1, total = weights(m_stat[...], y_stat[...])
    share = 1.0 / jnp.where(lane < HD // 2, total, 1.0)
    e0, e1 = lanes_of(y, e0 * share), lanes_of(y, e1 * share)
    first = y * seqs * group
    g_copies = []
    for i in range(blocks):
        y_copies[i].wait_recv()
        for r in range(span):
            b = i * span + r
            rows = pl.ds(b * group, group)
            mine = m_acc[pl.ds(pl.multiple_of(first + b * group, group), group), :]
            val = mine * e0[:, b:b + 1] + y_acc[rows, :] * e1[:, b:b + 1]
            att[core, rows, :] = val.astype(BF16).astype(F32)
        block = att.at[core, pl.ds(i * height, height)]
        copy = remote(block, block, g_send.at[i], g_recv.at[i], {'sp': partner})
        copy.start()
        g_copies.append(copy)
    for i in range(blocks):
        g_copies[i].wait_recv()
    for g in range(2):
        for j in range(group):
            n = g * group + j
            a_ref[:, n * HD:(n + 1) * HD] = att[g, pl.ds(j, seqs, stride=group), :].astype(BF16)
    w_copy.wait()

    chunks = part.shape[0]
    wide = part.shape[2]

    per_dot = 256 // wide

    def compute(j):
        val = jnp.dot(a_ref[...], w_buf[:, j * 256:(j + 1) * 256], preferred_element_type=F32)
        for n in range(per_dot):
            part[j * per_dot + n] = val[:, n * wide:(n + 1) * wide]

    def emit(half, side, i, ref):
        at = (pl.ds(pl.multiple_of(half * seqs, seqs), seqs), pl.ds(pl.multiple_of(side * width + i * wide, wide), wide))
        out_ref[at] = (h_ref[at].astype(F32) + ref[i]).astype(BF16)

    def e_copy(i):
        return remote(part.at[i], e_buf.at[i], e_send.at[i], e_recv.at[i], {'tp': hub_of_end})

    def b_copy(i):
        return remote(a_buf.at[i], b_buf.at[i], b_send.at[i], b_recv.at[i], {'tp': other_hub})

    def t_copy(i):
        return remote(tot.at[i], tot.at[i], t_send.at[i], t_recv.at[i], {'tp': end_of_hub})

    def y_copy(i):
        return remote(tot.at[i], y_buf.at[i], ys.at[i], yr.at[i], {'sp': cross})

    def p1_copy(i):
        return remote(tot.at[i], p1_buf.at[i], p1s.at[i], p1r.at[i], {'sp': partner})

    def p2_copy(i):
        return remote(y_buf.at[i], p2_buf.at[i], p2s.at[i], p2r.at[i], {'sp': partner})

    def spread(i):
        y_copy(i).start()
        p1_copy(i).start()
        emit(y, core, i, tot)

    def pass_on(i):
        y_copy(i).wait_recv()
        p2_copy(i).start()
        emit(1 - y, core, i, y_buf)

    @pl.when(is_hub)
    def _():
        lag, lag2 = 7, 15
        for j in range(chunks // per_dot):
            compute(j)
        for t in range(chunks + lag2):
            if t < chunks:
                e_copy(t).wait_recv()
                a_buf[t] = part[t] + e_buf[t]
                b_copy(t).start()
            i = t - lag
            if 0 <= i < chunks:
                b_copy(i).wait_recv()
                tot[i] = a_buf[i] + b_buf[i]
                t_copy(i).start()
                spread(i)
            i = t - lag2
            if 0 <= i < chunks:
                pass_on(i)
        for i in range(chunks):
            b_copy(i).wait_send()
            t_copy(i).wait_send()

    @pl.when(jnp.logical_not(is_hub))
    def _():
        lag = 8
        for j in range(chunks // per_dot + 1):
            if j < chunks // per_dot:
                compute(j)
            for n in range(per_dot):
                if j > 0:
                    e_copy((j - 1) * per_dot + n).start()
        for t in range(chunks + lag):
            if t < chunks:
                t_copy(t).wait_recv()
                spread(t)
            i = t - lag
            if 0 <= i < chunks:
                pass_on(i)
        for i in range(chunks):
            e_copy(i).wait_send()

    for i in range(chunks):
        p1_copy(i).wait_recv()
        emit(y, other, i, p1_buf)
        p2_copy(i).wait_recv()
        emit(1 - y, other, i, p2_buf)
    for i in range(chunks):
        y_copy(i).wait_send()
        p1_copy(i).wait_send()
        p2_copy(i).wait_send()
    st_copy.wait_send()
    sy_copy.wait_send()
    for copy in d_copies + y_copies + g_copies:
        copy.wait_send()


def solution(mesh):
    cache_spec = P('dp', 'sp', 'tp', None)
    hbm = pl.BlockSpec(memory_space=pltpu.HBM)
    vmem = pl.BlockSpec(memory_space=pltpu.VMEM)
    smem = pl.BlockSpec(memory_space=pltpu.SMEM)
    dma = pltpu.SemaphoreType.DMA

    def local_step(hidden, norm_scale, w_qkv, w_out, k_cache, v_cache, positions):
        n_seq, seq_local, kv_local, head_dim = k_cache.shape
        d = hidden.shape[1]
        rows = seq_local * kv_local
        heads = w_qkv.shape[1] // head_dim
        group = heads // kv_local - 2
        k_flat = k_cache.reshape(n_seq, rows, head_dim)
        v_flat = v_cache.reshape(n_seq, rows, head_dim)
        share = heads // 4
        in_hbm = [pltpu.with_memory_space_constraint(a, pltpu.HBM)
                  for a in (hidden, norm_scale.reshape(d // head_dim, head_dim), positions.reshape(1, n_seq), w_qkv, k_flat, v_flat)]
        cache_type = pltpu.VMEM((n_seq, rows, head_dim), BF16)
        table = pltpu.VMEM((n_seq, head_dim), F32)
        groups = [2, 2, share - 4]
        qkv, k_vmem, v_vmem = pl.pallas_call(
            qkv_kernel,
            out_shape=[pltpu.VMEM((4, share, n_seq, head_dim), F32), cache_type, cache_type],
            in_specs=[hbm] * 6,
            out_specs=[vmem, vmem, vmem],
            scratch_shapes=[
                pltpu.VMEM((n_seq, d), BF16), pltpu.VMEM((d // head_dim, head_dim), BF16), pltpu.VMEM((1, n_seq), jnp.int32),
                *[pltpu.VMEM((d, n * head_dim), BF16) for n in groups], pltpu.VMEM((n_seq, d), BF16), table, table,
                dma((3,)), dma((3, 2)), dma((2,)), *[dma((3,)) for _ in range(6)],
            ],
            compiler_params=pltpu.CompilerParams(collective_id=0, has_side_effects=True, vmem_limit_bytes=24 << 20),
            name='qkv',
        )(*in_hbm)
        qkv = qkv.reshape(heads, n_seq, head_dim)

        batch = 8
        k_out, v_out, acc, stat = pl.pallas_call(
            attention_kernel,
            out_shape=[
                jax.ShapeDtypeStruct(k_flat.shape, BF16), jax.ShapeDtypeStruct(v_flat.shape, BF16),
                pltpu.VMEM((2, n_seq, group, head_dim), F32), pltpu.VMEM((2, group, head_dim), F32),
            ],
            in_specs=[smem, vmem, vmem, vmem],
            out_specs=[hbm, hbm, vmem, vmem],
            scratch_shapes=[
                pltpu.VMEM((n_seq * 2 * group, head_dim), F32), pltpu.VMEM((batch * 2 * group, rows), F32),
                pltpu.VMEM((batch * 2 * group, rows), BF16), dma((2, 8)),
            ],
            compiler_params=pltpu.CompilerParams(vmem_limit_bytes=16 << 20),
            name='attention',
        )(positions, qkv, k_vmem, v_vmem)
        acc = acc.reshape(2, n_seq * group, head_dim)

        width = d // 2
        depth = w_out.shape[0]
        wide = CHUNK
        chunks = width // wide
        blocks = 4
        seqs = n_seq // 2
        slot = pltpu.VMEM((chunks, seqs, wide), F32)
        whole = pltpu.VMEM((n_seq * group, head_dim), F32)
        half = pltpu.VMEM((seqs * group, head_dim), F32)
        tile = pltpu.VMEM((group, head_dim), F32)
        h_out = pl.pallas_call(
            project_kernel,
            out_shape=jax.ShapeDtypeStruct((n_seq, d), BF16),
            in_specs=[vmem, vmem, vmem, hbm],
            out_specs=vmem,
            scratch_shapes=[
                pltpu.VMEM((depth, width), BF16), whole, tile, whole, tile, half, tile,
                pltpu.VMEM((2, seqs * group, head_dim), F32), pltpu.VMEM((seqs, depth), BF16),
                slot, slot, slot, slot, slot, slot, slot, slot,
                dma(()), dma((2,)), dma((2,)), dma((2 * blocks,)), dma((2 * blocks,)), *[dma((blocks,)) for _ in range(4)],
                *[dma((chunks,)) for _ in range(12)],
            ],
            compiler_params=pltpu.CompilerParams(collective_id=1, has_side_effects=True, vmem_limit_bytes=40 << 20),
            name='project',
        )(hidden, acc, stat, pltpu.with_memory_space_constraint(w_out, pltpu.HBM))
        return h_out, k_out.reshape(k_cache.shape), v_out.reshape(v_cache.shape)

    return jax.shard_map(
        local_step,
        mesh=mesh,
        in_specs=(P('dp', None), P(None), P(None, 'tp'), P('tp', None), cache_spec, cache_spec, P('dp')),
        out_specs=(P('dp', None), cache_spec, cache_spec),
        check_vma=False,
    )
```

```python
import math
import jax
import jax.numpy as jnp
from jax import lax
from jax.experimental import pallas as pl
from jax.experimental.pallas import tpu as pltpu
from jax.sharding import PartitionSpec as P

F32 = jnp.float32
BF16 = jnp.bfloat16
HD = 128
NEG = -3e38
FLOOR = -1e38
MESH_ID = pl.DeviceIdType.MESH
CHUNK = 128


def remote(src, dst, send_sem, recv_sem, device_id):
    return pltpu.make_async_remote_copy(
        src_ref=src, dst_ref=dst, send_sem=send_sem, recv_sem=recv_sem, device_id=device_id, device_id_type=MESH_ID
    )


def sp_peers():
    sp = lax.axis_index('sp')
    return sp, sp + 1 - 2 * lax.rem(sp, 2), lax.rem(sp + 2, 4)


def enter(peers):
    barrier = pltpu.get_barrier_semaphore()
    for peer in peers:
        pl.semaphore_signal(barrier, inc=1, device_id=peer, device_id_type=MESH_ID)
    pl.semaphore_wait(barrier, len(peers))


def qkv_kernel(h_hbm, scale_hbm, pos_hbm, w_hbm, kc_hbm, vc_hbm, qkv_ref, k_ref, v_ref,
               h_ref, scale_ref, pos_ref, w0_buf, w1_buf, w2_buf, u_ref, cos_ref, sin_ref,
               i_sem, w_sem, c_sem, a_send, a_recv, b_send, b_recv, f_send, f_recv):
    sp, partner, cross = sp_peers()
    n_seq, d = h_ref.shape
    ins = [pltpu.make_async_copy(src, dst, i_sem.at[i])
           for i, (src, dst) in enumerate(((pos_hbm, pos_ref), (h_hbm, h_ref), (scale_hbm, scale_ref)))]
    for copy in ins:
        copy.start()
    bufs = (w0_buf, w1_buf, w2_buf)
    width = sum(buf.shape[1] for buf in bufs)
    pieces = w_sem.shape[1]
    depth = d // pieces
    w_copies, first = [], 0
    for g, buf in enumerate(bufs):
        col = pl.multiple_of(sp * width + first, HD)
        first += buf.shape[1]

        def w_copy(i, g=g, buf=buf, col=col):
            rows = pl.ds(pl.multiple_of(i * depth, depth), depth)
            return pltpu.make_async_copy(w_hbm.at[rows, pl.ds(col, buf.shape[1])], buf.at[rows], w_sem.at[g, i])

        lax.fori_loop(0, pieces, lambda i, carry, w_copy=w_copy: (w_copy(i).start(), carry)[1], 0)
        w_copies.append([w_copy(i) for i in range(pieces)])
    enter([{'sp': partner}, {'sp': cross}])

    ins[0].wait()
    row_id = lax.broadcasted_iota(jnp.int32, (n_seq, n_seq), 0)
    col_id = lax.broadcasted_iota(jnp.int32, (n_seq, n_seq), 1)
    pos = jnp.sum(jnp.where(row_id == col_id, pos_ref[...].astype(F32), 0.0), axis=-1, keepdims=True)
    lane = lax.broadcasted_iota(jnp.int32, (n_seq, HD), 1)
    freq = lax.rem(lane, HD // 2).astype(F32)
    angles = pos * jnp.exp(freq * (-2.0 * math.log(500000.0) / HD))
    cos_ref[...] = jnp.cos(angles)
    sin_part = jnp.sin(angles)
    sin_ref[...] = jnp.where(lane < HD // 2, -sin_part, sin_part)

    ins[1].wait()
    tiles = d // HD

    def tile(k):
        return h_ref[:, k * HD:(k + 1) * HD].astype(F32)

    total = tile(0)
    for k in range(1, tiles):
        total += tile(k)
    mean = jnp.sum(total, axis=-1, keepdims=True) * (1.0 / d)
    total = jnp.zeros((n_seq, HD), F32)
    for k in range(tiles):
        centered = tile(k) - mean
        total += centered * centered
    inv = lax.rsqrt(jnp.sum(total, axis=-1, keepdims=True) * (1.0 / d) + 1e-5)
    ins[2].wait()
    scale_rows = scale_ref[...].astype(F32)
    for k in range(tiles):
        u_ref[:, k * HD:(k + 1) * HD] = ((tile(k) - mean) * inv * scale_rows[k:k + 1, :]).astype(BF16)

    cache_copies = [pltpu.make_async_copy(kc_hbm, k_ref, c_sem.at[0]), pltpu.make_async_copy(vc_hbm, v_ref, c_sem.at[1])]
    odd = lax.rem(sp, 2)
    heads = width // HD
    to_cross, to_partner, forward = [], [], []
    j = 0
    for g, buf in enumerate(bufs):
        acc = None
        for i in range(pieces):
            w_copies[g][i].wait()
            rows = slice(i * depth, (i + 1) * depth)
            if g >= 1 and i == 0:
                cache_copies[g - 1].start()
            part = jnp.dot(u_ref[:, rows], buf[rows, :], preferred_element_type=F32)
            acc = part if acc is None else acc + part
        proj = jnp.clip(acc.astype(BF16).astype(F32), -8.0, 8.0)
        n = buf.shape[1] // HD
        for r in range(n):
            val = proj[:, r * HD:(r + 1) * HD]
            rot = (val * cos_ref[...] + pltpu.roll(val, HD // 2, 1) * sin_ref[...]).astype(BF16).astype(F32)
            if j + r == heads - 1:
                rot = jnp.where(odd == 1, val, rot)
            qkv_ref[sp, j + r] = rot
        mine = qkv_ref.at[sp, pl.ds(j, n)]
        theirs = qkv_ref.at[cross, pl.ds(j, n)]
        to_cross.append(remote(mine, mine, a_send.at[g], a_recv.at[g], {'sp': cross}))
        to_partner.append(remote(mine, mine, b_send.at[g], b_recv.at[g], {'sp': partner}))
        forward.append(remote(theirs, theirs, f_send.at[g], f_recv.at[g], {'sp': partner}))
        to_cross[g].start()
        to_partner[g].start()
        j += n
    for g in range(len(bufs)):
        to_cross[g].wait_recv()
        forward[g].start()
    for copy in cache_copies:
        copy.wait()
    for g in range(len(bufs)):
        to_partner[g].wait()
        to_cross[g].wait_send()
        forward[g].wait()


def prepare_kernel(pos_ref, qkv_ref, k_ref, v_ref, q_ref, k_new, v_new):
    n_seq, rows, _ = k_ref.shape
    base = lax.axis_index('sp') * (rows // 2)
    n_q = q_ref.shape[0] // n_seq
    group = n_q // 2
    per_kv = group + 2

    tile = 16
    row_id = lax.broadcasted_iota(jnp.int32, (tile, HD), 0)
    at_once = 8

    def patch(i, carry):
        for r in range(at_once):
            b = i * at_once + r
            row = 2 * (pos_ref[b] - base)
            start = pl.multiple_of(jnp.clip(row // tile, 0, rows // tile - 1) * tile, tile)
            off = row - start
            for ref, new, slot in ((k_ref, k_new, group), (v_ref, v_new, group + 1)):
                block = ref[b, pl.ds(start, tile), :].astype(F32)
                one = qkv_ref[slot, pl.ds(b, 1), :]
                two = qkv_ref[per_kv + slot, pl.ds(b, 1), :]
                block = jnp.where(row_id == off, one, jnp.where(row_id == off + 1, two, block))
                new[b, pl.ds(start, tile), :] = block.astype(BF16)
        return carry

    lax.fori_loop(0, n_seq // at_once, patch, 0)
    for g in range(2):
        for j in range(group):
            q_ref[pl.ds(g * group + j, n_seq, stride=n_q), :] = qkv_ref[g * per_kv + j]


def finish_kernel(h_ref, k_ref, v_ref, h_out, k_out, v_out, h_sem, out_sem):
    pieces = out_sem.shape[1]
    span = k_ref.shape[0] // pieces
    copies = [pltpu.make_async_copy(h_ref, h_out, h_sem)]
    for i in range(pieces):
        for n, (src, dst) in enumerate(((k_ref, k_out), (v_ref, v_out))):
            at = pl.ds(i * span, span)
            copies.append(pltpu.make_async_copy(src.at[at], dst.at[at], out_sem.at[n, i]))
    for copy in copies:
        copy.start()
    for copy in copies:
        copy.wait()


def project_kernel(pos_ref, q_ref, k_ref, v_ref, h_ref, w_hbm, out_ref, w_buf, s_ref, p_ref, acc, d_acc, m_acc, y_acc, att, a_ref,
                   part, e_buf, a_buf, b_buf, tot, y_buf, p1_buf, p2_buf,
                   w_sem, d_send, d_recv, y_send, y_recv, g_send, g_recv,
                   e_send, e_recv, b_send, b_recv, t_send, t_recv, ys, yr, p1s, p1r, p2s, p2r):
    sp, partner, cross = sp_peers()
    core = lax.rem(sp, 2)
    other = 1 - core
    y = sp // 2
    z = lax.axis_index('tp')
    is_hub = (z == 1) | (z == 2)
    end_of_hub = 3 * (z - 1)
    hub_of_end = 1 + z // 2
    other_hub = 3 - z
    width = w_buf.shape[1]
    col = pl.multiple_of(core * width, HD)
    w_copy = pltpu.make_async_copy(w_hbm.at[:, pl.ds(col, width)], w_buf, w_sem)
    w_copy.start()

    barrier = pltpu.get_barrier_semaphore()
    for peer in ({'sp': partner}, {'sp': cross}):
        pl.semaphore_signal(barrier, inc=1, device_id=peer, device_id_type=MESH_ID)

    @pl.when(is_hub)
    def _():
        for peer in ({'tp': end_of_hub}, {'tp': other_hub}):
            pl.semaphore_signal(barrier, inc=1, device_id=peer, device_id_type=MESH_ID)

    @pl.when(jnp.logical_not(is_hub))
    def _():
        pl.semaphore_signal(barrier, inc=1, device_id={'tp': hub_of_end}, device_id_type=MESH_ID)

    n_seq, rows, _ = k_ref.shape
    n_q = q_ref.shape[0] // n_seq
    group = n_q // 2
    seqs = n_seq // 2
    units = acc.shape[0]
    span = n_seq // units
    height = span * group
    base = sp * (rows // 2)
    firsts = [(1 - y) * seqs, (1 - y) * seqs + span, y * seqs, y * seqs + span]
    col_id = lax.broadcasted_iota(jnp.int32, (n_q, rows), 1)
    head_id = lax.broadcasted_iota(jnp.int32, (n_q, rows), 0) // group
    col_key = jnp.where(lax.rem(col_id, 2) == head_id, col_id, 1 << 30)
    lane = lax.broadcasted_iota(jnp.int32, (n_q, HD), 1)
    low = lax.broadcasted_iota(jnp.int32, (group, HD), 1) < HD // 2
    upper = lax.broadcasted_iota(jnp.int32, (2 * n_q, HD), 0) < n_q
    factor = HD ** -0.5 * math.log2(math.e)
    batch = s_ref.shape[0] // n_q
    per_unit = span // batch
    steps = units * per_unit
    stats = [jnp.zeros((n_q, HD), F32) for _ in range(units)]

    def score(i):
        for r in range(0, batch, 2):
            b = firsts[i // per_unit] + (i % per_unit) * batch + r
            q = q_ref[pl.ds(pl.multiple_of(b * n_q, 2 * n_q), 2 * n_q), :]
            lhs = jnp.concatenate([jnp.where(upper, q, 0.0), jnp.where(upper, 0.0, q)], axis=1).astype(BF16)
            rhs = jnp.concatenate([k_ref[b], k_ref[b + 1]], axis=1)
            out = lax.dot_general(lhs, rhs, (((1,), (1,)), ((), ())), preferred_element_type=F32)
            for e in range(2):
                limit = 2 * (pos_ref[b + e] - base + 1)
                half = out[e * n_q:(e + 1) * n_q] * factor
                s_ref[(r + e) * n_q:(r + e + 1) * n_q, :] = jnp.where(col_key < limit, half, NEG)

    def soften(i):
        u = i // per_unit
        for r in range(batch):
            at = (i % per_unit) * batch + r
            scores = s_ref[r * n_q:(r + 1) * n_q, :]
            top = jnp.maximum(jnp.max(scores, axis=-1, keepdims=True), FLOOR)
            probs = jnp.exp2(scores - top)
            total = jnp.sum(probs, axis=-1, keepdims=True)
            p_ref[r * n_q:(r + 1) * n_q, :] = probs.astype(BF16)
            stats[u] = jnp.where(lane == at, top, jnp.where(lane == at + HD // 2, total, stats[u]))

    def weigh(i):
        u = i // per_unit
        for r in range(0, batch, 2):
            at = (i % per_unit) * batch + r
            b = firsts[u] + at
            rhs = jnp.concatenate([v_ref[b], v_ref[b + 1]], axis=1)
            out = jnp.dot(p_ref[r * n_q:(r + 2) * n_q, :], rhs, preferred_element_type=F32)
            for e in range(2):
                own = out[e * n_q:(e + 1) * n_q, e * HD:(e + 1) * HD]
                acc[u, 0, (at + e) * group:(at + e + 1) * group, :] = own[:group]
                acc[u, 1, (at + e) * group:(at + e + 1) * group, :] = own[group:]
        if i % per_unit == per_unit - 1:
            acc[u, 0, height:, :] = stats[u][:group]
            acc[u, 1, height:, :] = stats[u][group:]

    def weights(s0, s1):
        l0, l1 = pltpu.roll(s0, HD // 2, 1), pltpu.roll(s1, HD // 2, 1)
        top = jnp.maximum(s0, s1)
        e0, e1 = jnp.exp2(s0 - top), jnp.exp2(s1 - top)
        return top, e0, e1, l0 * e0 + l1 * e1

    def d_copy(u):
        return remote(acc.at[u, other], d_acc.at[u], d_send.at[u], d_recv.at[u], {'sp': partner})

    def m_copy(u):
        return remote(m_acc.at[u], y_acc.at[u], y_send.at[u], y_recv.at[u], {'sp': cross})

    def g_copy(u):
        block = att.at[core, pl.ds(u * height, height)]
        return remote(block, block, g_send.at[u], g_recv.at[u], {'sp': partner})

    def merge(u):
        d_copy(u).wait_recv()
        top, e0, e1, total = weights(acc[u, core, height:, :], d_acc[u, height:, :])
        m_acc[u, height:, :] = jnp.where(low, top, pltpu.roll(total, HD // 2, 1))
        for r in range(span):
            at = slice(r * group, (r + 1) * group)
            m_acc[u, at, :] = acc[u, core, at, :] * e0[:, r:r + 1] + d_acc[u, at, :] * e1[:, r:r + 1]
        if u < units // 2:
            m_copy(u).start()

    def settle(u):
        m_copy(u).wait_recv()
        own = units // 2 + u
        top, e0, e1, total = weights(m_acc[own, height:, :], y_acc[u, height:, :])
        share = 1.0 / jnp.where(low, total, 1.0)
        e0, e1 = e0 * share, e1 * share
        for r in range(span):
            at = slice(r * group, (r + 1) * group)
            val = m_acc[own, at, :] * e0[:, r:r + 1] + y_acc[u, at, :] * e1[:, r:r + 1]
            att[core, u * height + r * group:u * height + (r + 1) * group, :] = val.astype(BF16).astype(F32)
        g_copy(u).start()

    for i in range(-2, steps):
        if i >= 0:
            weigh(i)
        if 0 <= i + 1 < steps:
            soften(i + 1)
        if i + 2 < steps:
            score(i + 2)
        if i >= 0 and i % per_unit == per_unit - 1:
            u = i // per_unit
            if u == 0:
                @pl.when(is_hub)
                def _():
                    pl.semaphore_wait(barrier, 4)

                @pl.when(jnp.logical_not(is_hub))
                def _():
                    pl.semaphore_wait(barrier, 3)

            d_copy(u).start()
            if u > 0:
                merge(u - 1)
    settle(0)
    merge(units - 1)
    settle(1)
    for u in range(units // 2):
        g_copy(u).wait_recv()
    for g in range(2):
        for j in range(group):
            n = g * group + j
            a_ref[:, n * HD:(n + 1) * HD] = att[g, pl.ds(j, seqs, stride=group), :].astype(BF16)
    w_copy.wait()

    chunks = part.shape[0]
    wide = part.shape[2]

    per_dot = 256 // wide

    def compute(j):
        val = jnp.dot(a_ref[...], w_buf[:, j * 256:(j + 1) * 256], preferred_element_type=F32)
        for n in range(per_dot):
            part[j * per_dot + n] = val[:, n * wide:(n + 1) * wide]

    def emit(half, side, i, ref):
        at = (pl.ds(pl.multiple_of(half * seqs, seqs), seqs), pl.ds(pl.multiple_of(side * width + i * wide, wide), wide))
        out_ref[at] = (h_ref[at].astype(F32) + ref[i]).astype(BF16)

    def e_copy(i):
        return remote(part.at[i], e_buf.at[i], e_send.at[i], e_recv.at[i], {'tp': hub_of_end})

    def b_copy(i):
        return remote(a_buf.at[i], b_buf.at[i], b_send.at[i], b_recv.at[i], {'tp': other_hub})

    def t_copy(i):
        return remote(tot.at[i], tot.at[i], t_send.at[i], t_recv.at[i], {'tp': end_of_hub})

    def y_copy(i):
        return remote(tot.at[i], y_buf.at[i], ys.at[i], yr.at[i], {'sp': cross})

    def p1_copy(i):
        return remote(tot.at[i], p1_buf.at[i], p1s.at[i], p1r.at[i], {'sp': partner})

    def p2_copy(i):
        return remote(y_buf.at[i], p2_buf.at[i], p2s.at[i], p2r.at[i], {'sp': partner})

    def spread(i):
        y_copy(i).start()
        p1_copy(i).start()
        emit(y, core, i, tot)

    def pass_on(i):
        y_copy(i).wait_recv()
        p2_copy(i).start()
        emit(1 - y, core, i, y_buf)

    @pl.when(is_hub)
    def _():
        lag, lag2 = 7, 15
        for j in range(chunks // per_dot):
            compute(j)
        for t in range(chunks + lag2):
            if t < chunks:
                e_copy(t).wait_recv()
                a_buf[t] = part[t] + e_buf[t]
                b_copy(t).start()
            i = t - lag
            if 0 <= i < chunks:
                b_copy(i).wait_recv()
                tot[i] = a_buf[i] + b_buf[i]
                t_copy(i).start()
                spread(i)
            i = t - lag2
            if 0 <= i < chunks:
                pass_on(i)
        for i in range(chunks):
            b_copy(i).wait_send()
            t_copy(i).wait_send()

    @pl.when(jnp.logical_not(is_hub))
    def _():
        lag = 8
        for j in range(chunks // per_dot + 1):
            if j < chunks // per_dot:
                compute(j)
            for n in range(per_dot):
                if j > 0:
                    e_copy((j - 1) * per_dot + n).start()
        for t in range(chunks + lag):
            if t < chunks:
                t_copy(t).wait_recv()
                spread(t)
            i = t - lag
            if 0 <= i < chunks:
                pass_on(i)
        for i in range(chunks):
            e_copy(i).wait_send()

    for i in range(chunks):
        p1_copy(i).wait_recv()
        emit(y, other, i, p1_buf)
        p2_copy(i).wait_recv()
        emit(1 - y, other, i, p2_buf)
    for i in range(chunks):
        y_copy(i).wait_send()
        p1_copy(i).wait_send()
        p2_copy(i).wait_send()
    for u in range(units):
        d_copy(u).wait_send()
    for u in range(units // 2):
        m_copy(u).wait_send()
        g_copy(u).wait_send()


def solution(mesh):
    cache_spec = P('dp', 'sp', 'tp', None)
    hbm = pl.BlockSpec(memory_space=pltpu.HBM)
    vmem = pl.BlockSpec(memory_space=pltpu.VMEM)
    smem = pl.BlockSpec(memory_space=pltpu.SMEM)
    dma = pltpu.SemaphoreType.DMA

    def local_step(hidden, norm_scale, w_qkv, w_out, k_cache, v_cache, positions):
        n_seq, seq_local, kv_local, head_dim = k_cache.shape
        d = hidden.shape[1]
        rows = seq_local * kv_local
        heads = w_qkv.shape[1] // head_dim
        group = heads // kv_local - 2
        k_flat = k_cache.reshape(n_seq, rows, head_dim)
        v_flat = v_cache.reshape(n_seq, rows, head_dim)
        share = heads // 4
        in_hbm = [pltpu.with_memory_space_constraint(a, pltpu.HBM)
                  for a in (hidden, norm_scale.reshape(d // head_dim, head_dim), positions.reshape(1, n_seq), w_qkv, k_flat, v_flat)]
        cache_type = pltpu.VMEM((n_seq, rows, head_dim), BF16)
        table = pltpu.VMEM((n_seq, head_dim), F32)
        groups = [2, 2, share - 4]
        qkv, k_vmem, v_vmem = pl.pallas_call(
            qkv_kernel,
            out_shape=[pltpu.VMEM((4, share, n_seq, head_dim), F32), cache_type, cache_type],
            in_specs=[hbm] * 6,
            out_specs=[vmem, vmem, vmem],
            scratch_shapes=[
                pltpu.VMEM((n_seq, d), BF16), pltpu.VMEM((d // head_dim, head_dim), BF16), pltpu.VMEM((1, n_seq), jnp.int32),
                *[pltpu.VMEM((d, n * head_dim), BF16) for n in groups], pltpu.VMEM((n_seq, d), BF16), table, table,
                dma((3,)), dma((3, 2)), dma((2,)), *[dma((3,)) for _ in range(6)],
            ],
            compiler_params=pltpu.CompilerParams(collective_id=0, has_side_effects=True, vmem_limit_bytes=24 << 20),
            name='qkv',
        )(*in_hbm)
        qkv = qkv.reshape(heads, n_seq, head_dim)

        query, k_vmem, v_vmem = pl.pallas_call(
            prepare_kernel,
            out_shape=[pltpu.VMEM((n_seq * 2 * group, head_dim), F32), cache_type, cache_type],
            in_specs=[smem, vmem, vmem, vmem],
            out_specs=[vmem, vmem, vmem],
            input_output_aliases={2: 1, 3: 2},
            compiler_params=pltpu.CompilerParams(vmem_limit_bytes=8 << 20),
            name='prepare',
        )(positions, qkv, k_vmem, v_vmem)

        width = d // 2
        depth = w_out.shape[0]
        wide = CHUNK
        chunks = width // wide
        batch, units = 8, 4
        seqs = n_seq // 2
        block = n_seq // units * group
        slot = pltpu.VMEM((chunks, seqs, wide), F32)
        h_new = pl.pallas_call(
            project_kernel,
            out_shape=pltpu.VMEM((n_seq, d), BF16),
            in_specs=[smem, vmem, vmem, vmem, vmem, hbm],
            out_specs=vmem,
            scratch_shapes=[
                pltpu.VMEM((depth, width), BF16),
                pltpu.VMEM((batch * 2 * group, rows), F32), pltpu.VMEM((batch * 2 * group, rows), BF16),
                pltpu.VMEM((units, 2, block + group, head_dim), F32), pltpu.VMEM((units, block + group, head_dim), F32),
                pltpu.VMEM((units, block + group, head_dim), F32), pltpu.VMEM((units // 2, block + group, head_dim), F32),
                pltpu.VMEM((2, seqs * group, head_dim), F32), pltpu.VMEM((seqs, depth), BF16),
                slot, slot, slot, slot, slot, slot, slot, slot,
                dma(()), dma((units,)), dma((units,)), *[dma((units // 2,)) for _ in range(4)],
                *[dma((chunks,)) for _ in range(12)],
            ],
            compiler_params=pltpu.CompilerParams(collective_id=1, has_side_effects=True, vmem_limit_bytes=30 << 20),
            name='project',
        )(positions, query, k_vmem, v_vmem, hidden, pltpu.with_memory_space_constraint(w_out, pltpu.HBM))

        h_out, k_out, v_out = pl.pallas_call(
            finish_kernel,
            out_shape=[jax.ShapeDtypeStruct(a.shape, BF16) for a in (hidden, k_flat, v_flat)],
            in_specs=[vmem, vmem, vmem],
            out_specs=[hbm, hbm, hbm],
            scratch_shapes=[dma(()), dma((2, 8))],
            compiler_params=pltpu.CompilerParams(vmem_limit_bytes=2 << 20),
            name='finish',
        )(h_new, k_vmem, v_vmem)
        return h_out, k_out.reshape(k_cache.shape), v_out.reshape(v_cache.shape)

    return jax.shard_map(
        local_step,
        mesh=mesh,
        in_specs=(P('dp', None), P(None), P(None, 'tp'), P('tp', None), cache_spec, cache_spec, P('dp')),
        out_specs=(P('dp', None), cache_spec, cache_spec),
        check_vma=False,
    )
```

```python
import functools
import math
import jax
import jax.numpy as jnp
from jax import lax
from jax.experimental import pallas as pl
from jax.experimental.pallas import tpu as pltpu
from jax.sharding import PartitionSpec as P

F32 = jnp.float32
BF16 = jnp.bfloat16
HD = 128
NEG = -3e38
FLOOR = -1e38
MESH_ID = pl.DeviceIdType.MESH
CHUNK = 128


def remote(src, dst, send_sem, recv_sem, device_id):
    return pltpu.make_async_remote_copy(
        src_ref=src, dst_ref=dst, send_sem=send_sem, recv_sem=recv_sem, device_id=device_id, device_id_type=MESH_ID
    )


def sp_peers():
    sp = lax.axis_index('sp')
    return sp, sp + 1 - 2 * lax.rem(sp, 2), lax.rem(sp + 2, 4)


def enter(peers):
    barrier = pltpu.get_barrier_semaphore()
    for peer in peers:
        pl.semaphore_signal(barrier, inc=1, device_id=peer, device_id_type=MESH_ID)
    pl.semaphore_wait(barrier, len(peers))


def qkv_kernel(h_hbm, scale_hbm, pos_hbm, w_hbm, kc_hbm, vc_hbm, qkv_ref, k_ref, v_ref,
               h_ref, scale_ref, pos_ref, w0_buf, w1_buf, w2_buf, u_ref, cos_ref, sin_ref,
               i_sem, w_sem, c_sem, a_send, a_recv, b_send, b_recv, f_send, f_recv):
    sp, partner, cross = sp_peers()
    n_seq, d = h_ref.shape
    ins = [pltpu.make_async_copy(src, dst, i_sem.at[i])
           for i, (src, dst) in enumerate(((pos_hbm, pos_ref), (h_hbm, h_ref), (scale_hbm, scale_ref)))]
    for copy in ins:
        copy.start()
    bufs = (w0_buf, w1_buf, w2_buf)
    width = sum(buf.shape[1] for buf in bufs)
    pieces = w_sem.shape[1]
    depth = d // pieces
    w_copies, first = [], 0
    for g, buf in enumerate(bufs):
        col = pl.multiple_of(sp * width + first, HD)
        first += buf.shape[1]

        def w_copy(i, g=g, buf=buf, col=col):
            rows = pl.ds(pl.multiple_of(i * depth, depth), depth)
            return pltpu.make_async_copy(w_hbm.at[rows, pl.ds(col, buf.shape[1])], buf.at[rows], w_sem.at[g, i])

        lax.fori_loop(0, pieces, lambda i, carry, w_copy=w_copy: (w_copy(i).start(), carry)[1], 0)
        w_copies.append([w_copy(i) for i in range(pieces)])
    enter([{'sp': partner}, {'sp': cross}])

    ins[0].wait()
    row_id = lax.broadcasted_iota(jnp.int32, (n_seq, n_seq), 0)
    col_id = lax.broadcasted_iota(jnp.int32, (n_seq, n_seq), 1)
    pos = jnp.sum(jnp.where(row_id == col_id, pos_ref[...].astype(F32), 0.0), axis=-1, keepdims=True)
    lane = lax.broadcasted_iota(jnp.int32, (n_seq, HD), 1)
    freq = lax.rem(lane, HD // 2).astype(F32)
    angles = pos * jnp.exp(freq * (-2.0 * math.log(500000.0) / HD))
    cos_ref[...] = jnp.cos(angles)
    sin_part = jnp.sin(angles)
    sin_ref[...] = jnp.where(lane < HD // 2, -sin_part, sin_part)

    ins[1].wait()
    tiles = d // HD

    def tile(k):
        return h_ref[:, k * HD:(k + 1) * HD].astype(F32)

    total = tile(0)
    for k in range(1, tiles):
        total += tile(k)
    mean = jnp.sum(total, axis=-1, keepdims=True) * (1.0 / d)
    total = jnp.zeros((n_seq, HD), F32)
    for k in range(tiles):
        centered = tile(k) - mean
        total += centered * centered
    inv = lax.rsqrt(jnp.sum(total, axis=-1, keepdims=True) * (1.0 / d) + 1e-5)
    ins[2].wait()
    scale_rows = scale_ref[...].astype(F32)
    for k in range(tiles):
        u_ref[:, k * HD:(k + 1) * HD] = ((tile(k) - mean) * inv * scale_rows[k:k + 1, :]).astype(BF16)

    cache_copies = [pltpu.make_async_copy(kc_hbm, k_ref, c_sem.at[0]), pltpu.make_async_copy(vc_hbm, v_ref, c_sem.at[1])]
    odd = lax.rem(sp, 2)
    heads = width // HD
    to_cross, to_partner, forward = [], [], []
    j = 0
    for g, buf in enumerate(bufs):
        acc = None
        for i in range(pieces):
            w_copies[g][i].wait()
            rows = slice(i * depth, (i + 1) * depth)
            if g >= 1 and i == 0:
                cache_copies[g - 1].start()
            part = jnp.dot(u_ref[:, rows], buf[rows, :], preferred_element_type=F32)
            acc = part if acc is None else acc + part
        proj = jnp.clip(acc.astype(BF16).astype(F32), -8.0, 8.0)
        n = buf.shape[1] // HD
        for r in range(n):
            val = proj[:, r * HD:(r + 1) * HD]
            rot = (val * cos_ref[...] + pltpu.roll(val, HD // 2, 1) * sin_ref[...]).astype(BF16).astype(F32)
            if j + r == heads - 1:
                rot = jnp.where(odd == 1, val, rot)
            qkv_ref[sp, j + r] = rot
        mine = qkv_ref.at[sp, pl.ds(j, n)]
        theirs = qkv_ref.at[cross, pl.ds(j, n)]
        to_cross.append(remote(mine, mine, a_send.at[g], a_recv.at[g], {'sp': cross}))
        to_partner.append(remote(mine, mine, b_send.at[g], b_recv.at[g], {'sp': partner}))
        forward.append(remote(theirs, theirs, f_send.at[g], f_recv.at[g], {'sp': partner}))
        to_cross[g].start()
        to_partner[g].start()
        j += n
    for g in range(len(bufs)):
        to_cross[g].wait_recv()
        forward[g].start()
    for copy in cache_copies:
        copy.wait()
    for g in range(len(bufs)):
        to_partner[g].wait()
        to_cross[g].wait_send()
        forward[g].wait()


def attention_kernel(pos_ref, qkv_ref, k_ref, v_ref, k_out, v_out, acc_ref, stat_ref, q_ref, s_ref, p_ref, out_sem):
    n_seq, rows, _ = k_ref.shape
    seq_local = rows // 2
    group = acc_ref.shape[2]
    base = lax.axis_index('sp') * seq_local
    per_kv = group + 2
    n_q = 2 * group

    tile = 16
    row_id = lax.broadcasted_iota(jnp.int32, (tile, HD), 0)
    at_once = 8

    def patch(i, carry):
        for r in range(at_once):
            b = i * at_once + r
            row = 2 * (pos_ref[b] - base)
            start = pl.multiple_of(jnp.clip(row // tile, 0, rows // tile - 1) * tile, tile)
            off = row - start
            for ref, slot in ((k_ref, group), (v_ref, group + 1)):
                block = ref[b, pl.ds(start, tile), :].astype(F32)
                one = qkv_ref[slot, pl.ds(b, 1), :]
                two = qkv_ref[per_kv + slot, pl.ds(b, 1), :]
                block = jnp.where(row_id == off, one, jnp.where(row_id == off + 1, two, block))
                ref[b, pl.ds(start, tile), :] = block.astype(BF16)
        return carry

    def out_copies(i):
        span = pl.ds(i * at_once, at_once)
        return [pltpu.make_async_copy(src.at[span], dst.at[span], out_sem.at[n, i])
                for n, (src, dst) in enumerate(((k_ref, k_out), (v_ref, v_out)))]

    def patch_and_write(i, carry):
        patch(i, carry)
        for copy in out_copies(i - 1):
            copy.start()
        return carry

    pieces = n_seq // at_once
    patch(0, 0)
    lax.fori_loop(1, pieces, patch_and_write, 0)
    for g in range(2):
        for j in range(group):
            q_ref[pl.ds(g * group + j, n_seq, stride=n_q), :] = qkv_ref[g * per_kv + j]
    for copy in out_copies(pieces - 1):
        copy.start()

    col_id = lax.broadcasted_iota(jnp.int32, (n_q, rows), 1)
    head_id = lax.broadcasted_iota(jnp.int32, (n_q, rows), 0) // group
    col_key = jnp.where(lax.rem(col_id, 2) == head_id, col_id, 1 << 30)
    lane = lax.broadcasted_iota(jnp.int32, (n_q, HD), 1)
    upper = lax.broadcasted_iota(jnp.int32, (2 * n_q, HD), 0) < n_q
    factor = HD ** -0.5 * math.log2(math.e)
    pairs = s_ref.shape[0] // (2 * n_q)
    batch = 2 * pairs

    def score(i):
        for r in range(pairs):
            b = i * batch + 2 * r
            q = q_ref[pl.ds(pl.multiple_of(b * n_q, 2 * n_q), 2 * n_q), :]
            lhs = jnp.concatenate([jnp.where(upper, q, 0.0), jnp.where(upper, 0.0, q)], axis=1).astype(BF16)
            rhs = jnp.concatenate([k_ref[b], k_ref[b + 1]], axis=1)
            out = lax.dot_general(lhs, rhs, (((1,), (1,)), ((), ())), preferred_element_type=F32)
            for e in range(2):
                limit = 2 * (pos_ref[b + e] - base + 1)
                half = out[e * n_q:(e + 1) * n_q] * factor
                s_ref[(2 * r + e) * n_q:(2 * r + e + 1) * n_q, :] = jnp.where(col_key < limit, half, NEG)

    def soften(i, stats):
        for r in range(batch):
            b = i * batch + r
            scores = s_ref[r * n_q:(r + 1) * n_q, :]
            top = jnp.maximum(jnp.max(scores, axis=-1, keepdims=True), FLOOR)
            probs = jnp.exp2(scores - top)
            total = jnp.sum(probs, axis=-1, keepdims=True)
            p_ref[r * n_q:(r + 1) * n_q, :] = probs.astype(BF16)
            stats = jnp.where(lane == b, top, jnp.where(lane == b + n_seq, total, stats))
        return stats

    def weigh(i):
        for r in range(pairs):
            b = i * batch + 2 * r
            rhs = jnp.concatenate([v_ref[b], v_ref[b + 1]], axis=1)
            out = jnp.dot(p_ref[2 * r * n_q:(2 * r + 2) * n_q, :], rhs, preferred_element_type=F32)
            for e in range(2):
                own = out[e * n_q:(e + 1) * n_q, e * HD:(e + 1) * HD]
                acc_ref[0, b + e] = own[:group]
                acc_ref[1, b + e] = own[group:]

    steps = n_seq // batch
    stats = jnp.zeros((n_q, HD), F32)
    score(0)
    stats = soften(0, stats)
    score(1)

    def step(i, stats):
        weigh(i)
        stats = soften(i + 1, stats)
        score(i + 2)
        return stats

    stats = lax.fori_loop(0, steps - 2, step, stats)
    weigh(steps - 2)
    stats = soften(steps - 1, stats)
    weigh(steps - 1)
    stat_ref[0] = stats[:group]
    stat_ref[1] = stats[group:]
    for i in range(pieces):
        for copy in out_copies(i):
            copy.wait()


def project_kernel(split, h_ref, acc_ref, stat_ref, w_hbm, out_ref, w_buf, d_acc, d_stat, m_acc, m_stat, y_acc, y_stat, att, a_ref,
                   part, e_buf, a_buf, b_buf, tot, y_buf, p1_buf, p2_buf,
                   w_sem, st_send, st_recv, d_send, d_recv, y_send, y_recv, g_send, g_recv,
                   e_send, e_recv, b_send, b_recv, t_send, t_recv, ys, yr, p1s, p1r, p2s, p2r):
    sp, partner, cross = sp_peers()
    core = lax.rem(sp, 2)
    y = sp // 2
    z = lax.axis_index('tp')
    is_hub = (z == 1) | (z == 2)
    end_of_hub = 3 * (z - 1)
    hub_of_end = 1 + z // 2
    other_hub = 3 - z
    few, many = split
    wide = part.shape[2]

    def on_side(side, then):
        for c, n in ((0, few), (1, many)):
            @pl.when(side == c)
            def _(c=c, n=n):
                then(c, n)

    def w_copy(c, n):
        return pltpu.make_async_copy(w_hbm.at[:, pl.ds(c * few * wide, n * wide)], w_buf.at[:, pl.ds(0, n * wide)], w_sem)

    on_side(core, lambda c, n: w_copy(c, n).start())

    barrier = pltpu.get_barrier_semaphore()
    for peer in ({'sp': partner}, {'sp': cross}):
        pl.semaphore_signal(barrier, inc=1, device_id=peer, device_id_type=MESH_ID)

    @pl.when(is_hub)
    def _():
        for peer in ({'tp': end_of_hub}, {'tp': other_hub}):
            pl.semaphore_signal(barrier, inc=1, device_id=peer, device_id_type=MESH_ID)
        pl.semaphore_wait(barrier, 4)

    @pl.when(jnp.logical_not(is_hub))
    def _():
        pl.semaphore_signal(barrier, inc=1, device_id={'tp': hub_of_end}, device_id_type=MESH_ID)
        pl.semaphore_wait(barrier, 3)

    group = stat_ref.shape[1]
    seqs = out_ref.shape[0] // 2
    blocks = y_send.shape[0]
    span = seqs // blocks
    height = span * group
    other = 1 - core
    st_copy = remote(stat_ref.at[other], d_stat, st_send.at[0], st_recv.at[0], {'sp': partner})
    st_copy.start()

    def rows_of(half, i):
        return pl.ds(pl.multiple_of((half * blocks + i) * height, height), height)

    d_copies = []
    for n in range(2 * blocks):
        rows = rows_of(1 - y if n < blocks else y, n % blocks)
        copy = remote(acc_ref.at[other, rows], d_acc.at[rows], d_send.at[n], d_recv.at[n], {'sp': partner})
        copy.start()
        d_copies.append(copy)
    st_copy.wait_recv()
    lane = lax.broadcasted_iota(jnp.int32, (group, HD), 1)

    def weights(s0, s1):
        l0, l1 = pltpu.roll(s0, HD // 2, 1), pltpu.roll(s1, HD // 2, 1)
        top = jnp.maximum(s0, s1)
        e0, e1 = jnp.exp2(s0 - top), jnp.exp2(s1 - top)
        return top, e0, e1, l0 * e0 + l1 * e1

    def lanes_of(half, val):
        return jnp.where(half == 0, val, pltpu.roll(val, HD - seqs, 1))

    top, e0, e1, total = weights(stat_ref[core], d_stat[...])
    m_stat[...] = jnp.where(lane < HD // 2, top, pltpu.roll(total, HD // 2, 1))
    sy_copy = remote(m_stat, y_stat, st_send.at[1], st_recv.at[1], {'sp': cross})
    y_copies = []
    for n in range(2 * blocks):
        half, i = (1 - y if n < blocks else y), n % blocks
        d_copies[n].wait_recv()
        f0, f1 = lanes_of(half, e0), lanes_of(half, e1)
        first = half * seqs * group
        for r in range(span):
            b = i * span + r
            rows = pl.ds(pl.multiple_of(first + b * group, group), group)
            m_acc[rows, :] = acc_ref[core, rows, :] * f0[:, b:b + 1] + d_acc[rows, :] * f1[:, b:b + 1]
        if n == 0:
            sy_copy.start()
        if n < blocks:
            copy = remote(m_acc.at[rows_of(half, i)], y_acc.at[pl.ds(i * height, height)], y_send.at[i], y_recv.at[i], {'sp': cross})
            copy.start()
            y_copies.append(copy)
    sy_copy.wait_recv()
    top, e0, e1, total = weights(m_stat[...], y_stat[...])
    share = 1.0 / jnp.where(lane < HD // 2, total, 1.0)
    e0, e1 = lanes_of(y, e0 * share), lanes_of(y, e1 * share)
    first = y * seqs * group
    def g_copy(i):
        block = att.at[core, pl.ds(i * height, height)]
        return remote(block, block, g_send.at[i], g_recv.at[i], {'sp': partner})

    def settle(i):
        y_copies[i].wait_recv()
        for r in range(span):
            b = i * span + r
            rows = pl.ds(b * group, group)
            mine = m_acc[pl.ds(pl.multiple_of(first + b * group, group), group), :]
            val = mine * e0[:, b:b + 1] + y_acc[rows, :] * e1[:, b:b + 1]
            att[core, rows, :] = val.astype(BF16).astype(F32)
        g_copy(i).start()

    n_groups = 2
    tall = seqs // n_groups
    per_group = blocks // n_groups

    def gather(g):
        for i in range(per_group):
            g_copy(g * per_group + i).wait_recv()
        for side in range(2):
            for j in range(group):
                n = side * group + j
                val = att[side, pl.ds(g * tall * group + j, tall, stride=group), :]
                a_ref[g * tall:(g + 1) * tall, n * HD:(n + 1) * HD] = val.astype(BF16)

    def guard(i, side, then):
        if i % many < few:
            then(i)
        else:
            @pl.when(side == 1)
            def _():
                then(i)

    chunks = n_groups * many

    def compute(i):
        g, j = i // many, i % many
        part[i] = jnp.dot(a_ref[g * tall:(g + 1) * tall, :], w_buf[:, j * wide:(j + 1) * wide], preferred_element_type=F32)

    def emit(half, side, i, ref):
        g, j = i // many, i % many
        at = (pl.ds(pl.multiple_of(half * seqs + g * tall, tall), tall), pl.ds(pl.multiple_of((side * few + j) * wide, wide), wide))
        out_ref[at] = (h_ref[at].astype(F32) + ref[i]).astype(BF16)

    def e_copy(i):
        return remote(part.at[i], e_buf.at[i], e_send.at[i], e_recv.at[i], {'tp': hub_of_end})

    def b_copy(i):
        return remote(a_buf.at[i], b_buf.at[i], b_send.at[i], b_recv.at[i], {'tp': other_hub})

    def t_copy(i):
        return remote(tot.at[i], tot.at[i], t_send.at[i], t_recv.at[i], {'tp': end_of_hub})

    def y_copy(i):
        return remote(tot.at[i], y_buf.at[i], ys.at[i], yr.at[i], {'sp': cross})

    def p1_copy(i):
        return remote(tot.at[i], p1_buf.at[i], p1s.at[i], p1r.at[i], {'sp': partner})

    def p2_copy(i):
        return remote(y_buf.at[i], p2_buf.at[i], p2s.at[i], p2r.at[i], {'sp': partner})

    def spread(i):
        y_copy(i).start()
        p1_copy(i).start()
        emit(y, core, i, tot)

    def pass_on(i):
        y_copy(i).wait_recv()
        p2_copy(i).start()
        emit(1 - y, core, i, y_buf)

    def add_end(i):
        e_copy(i).wait_recv()
        a_buf[i] = part[i] + e_buf[i]
        b_copy(i).start()

    def add_hub(i):
        b_copy(i).wait_recv()
        tot[i] = a_buf[i] + b_buf[i]
        t_copy(i).start()
        spread(i)

    def take(i):
        t_copy(i).wait_recv()
        spread(i)

    def send_end(i):
        e_copy(i).start()

    def at_core(i, then):
        if 0 <= i < chunks:
            guard(i, core, then)

    settle(0)
    settle(1)
    settle(2)
    gather(0)
    on_side(core, lambda c, n: w_copy(c, n).wait())
    early = 4

    @pl.when(is_hub)
    def _():
        lag, lag2 = 7, 15
        for i in range(early):
            at_core(i, compute)
        settle(3)
        for i in range(early, few):
            at_core(i, compute)

        @pl.when(core == 1)
        def _():
            for i in range(few, many):
                compute(i)

        gather(1)
        for t in range(chunks + lag2):
            if t < many:
                at_core(t + many, compute)
            at_core(t, add_end)
            at_core(t - lag, add_hub)
            at_core(t - lag2, pass_on)
        for i in range(chunks):
            guard(i, core, lambda i: (b_copy(i).wait_send(), t_copy(i).wait_send()))

    @pl.when(jnp.logical_not(is_hub))
    def _():
        lag = 8

        def project(first_one, last_one):
            for i in range(first_one, last_one + 1):
                if i < last_one:
                    compute(i)
                if i > first_one:
                    send_end(i - 1)

        for g in range(n_groups):
            if g == 0:
                project(0, early)
                settle(3)
                project(early, few)
            else:
                gather(1)
                project(many, many + few)

            @pl.when(core == 1)
            def _(g=g):
                project(g * many + few, (g + 1) * many)

        for t in range(chunks + lag):
            at_core(t, take)
            at_core(t - lag, pass_on)
        for i in range(chunks):
            guard(i, core, lambda i: e_copy(i).wait_send())

    def finish(i):
        p1_copy(i).wait_recv()
        emit(y, other, i, p1_buf)
        p2_copy(i).wait_recv()
        emit(1 - y, other, i, p2_buf)

    for i in range(chunks):
        guard(i, other, finish)
    for i in range(chunks):
        guard(i, core, lambda i: (y_copy(i).wait_send(), p1_copy(i).wait_send(), p2_copy(i).wait_send()))
    st_copy.wait_send()
    sy_copy.wait_send()
    for copy in d_copies + y_copies:
        copy.wait_send()
    for i in range(blocks):
        g_copy(i).wait_send()


def solution(mesh):
    cache_spec = P('dp', 'sp', 'tp', None)
    hbm = pl.BlockSpec(memory_space=pltpu.HBM)
    vmem = pl.BlockSpec(memory_space=pltpu.VMEM)
    smem = pl.BlockSpec(memory_space=pltpu.SMEM)
    dma = pltpu.SemaphoreType.DMA

    def local_step(hidden, norm_scale, w_qkv, w_out, k_cache, v_cache, positions):
        n_seq, seq_local, kv_local, head_dim = k_cache.shape
        d = hidden.shape[1]
        rows = seq_local * kv_local
        heads = w_qkv.shape[1] // head_dim
        group = heads // kv_local - 2
        k_flat = k_cache.reshape(n_seq, rows, head_dim)
        v_flat = v_cache.reshape(n_seq, rows, head_dim)
        share = heads // 4
        in_hbm = [pltpu.with_memory_space_constraint(a, pltpu.HBM)
                  for a in (hidden, norm_scale.reshape(d // head_dim, head_dim), positions.reshape(1, n_seq), w_qkv, k_flat, v_flat)]
        cache_type = pltpu.VMEM((n_seq, rows, head_dim), BF16)
        table = pltpu.VMEM((n_seq, head_dim), F32)
        groups = [2, 2, share - 4]
        qkv, k_vmem, v_vmem = pl.pallas_call(
            qkv_kernel,
            out_shape=[pltpu.VMEM((4, share, n_seq, head_dim), F32), cache_type, cache_type],
            in_specs=[hbm] * 6,
            out_specs=[vmem, vmem, vmem],
            scratch_shapes=[
                pltpu.VMEM((n_seq, d), BF16), pltpu.VMEM((d // head_dim, head_dim), BF16), pltpu.VMEM((1, n_seq), jnp.int32),
                *[pltpu.VMEM((d, n * head_dim), BF16) for n in groups], pltpu.VMEM((n_seq, d), BF16), table, table,
                dma((3,)), dma((3, 2)), dma((2,)), *[dma((3,)) for _ in range(6)],
            ],
            compiler_params=pltpu.CompilerParams(collective_id=0, has_side_effects=True, vmem_limit_bytes=24 << 20),
            name='qkv',
        )(*in_hbm)
        qkv = qkv.reshape(heads, n_seq, head_dim)

        batch = 8
        k_out, v_out, acc, stat = pl.pallas_call(
            attention_kernel,
            out_shape=[
                jax.ShapeDtypeStruct(k_flat.shape, BF16), jax.ShapeDtypeStruct(v_flat.shape, BF16),
                pltpu.VMEM((2, n_seq, group, head_dim), F32), pltpu.VMEM((2, group, head_dim), F32),
            ],
            in_specs=[smem, vmem, vmem, vmem],
            out_specs=[hbm, hbm, vmem, vmem],
            scratch_shapes=[
                pltpu.VMEM((n_seq * 2 * group, head_dim), F32), pltpu.VMEM((batch * 2 * group, rows), F32),
                pltpu.VMEM((batch * 2 * group, rows), BF16), dma((2, 8)),
            ],
            compiler_params=pltpu.CompilerParams(vmem_limit_bytes=16 << 20),
            name='attention',
        )(positions, qkv, k_vmem, v_vmem)
        acc = acc.reshape(2, n_seq * group, head_dim)

        depth = w_out.shape[0]
        wide = 2 * CHUNK
        few = d // wide * 13 // 32
        many = d // wide - few
        chunks = 2 * many
        blocks = 4
        seqs = n_seq // 2
        slot = pltpu.VMEM((chunks, seqs // 2, wide), F32)
        whole = pltpu.VMEM((n_seq * group, head_dim), F32)
        half = pltpu.VMEM((seqs * group, head_dim), F32)
        tile = pltpu.VMEM((group, head_dim), F32)
        h_out = pl.pallas_call(
            functools.partial(project_kernel, (few, many)),
            out_shape=jax.ShapeDtypeStruct((n_seq, d), BF16),
            in_specs=[vmem, vmem, vmem, hbm],
            out_specs=vmem,
            scratch_shapes=[
                pltpu.VMEM((depth, many * wide), BF16), whole, tile, whole, tile, half, tile,
                pltpu.VMEM((2, seqs * group, head_dim), F32), pltpu.VMEM((seqs, depth), BF16),
                slot, slot, slot, slot, slot, slot, slot, slot,
                dma(()), dma((2,)), dma((2,)), dma((2 * blocks,)), dma((2 * blocks,)), *[dma((blocks,)) for _ in range(4)],
                *[dma((chunks,)) for _ in range(12)],
            ],
            compiler_params=pltpu.CompilerParams(collective_id=1, has_side_effects=True, vmem_limit_bytes=40 << 20),
            name='project',
        )(hidden, acc, stat, pltpu.with_memory_space_constraint(w_out, pltpu.HBM))
        return h_out, k_out.reshape(k_cache.shape), v_out.reshape(v_cache.shape)

    return jax.shard_map(
        local_step,
        mesh=mesh,
        in_specs=(P('dp', None), P(None), P(None, 'tp'), P('tp', None), cache_spec, cache_spec, P('dp')),
        out_specs=(P('dp', None), cache_spec, cache_spec),
        check_vma=False,
    )
```

```python
import math
import jax
import jax.numpy as jnp
from jax import lax
from jax.experimental import pallas as pl
from jax.experimental.pallas import tpu as pltpu
from jax.sharding import PartitionSpec as P

F32 = jnp.float32
BF16 = jnp.bfloat16
HD = 128
NEG = -3e38
FLOOR = -1e38
MESH_ID = pl.DeviceIdType.MESH
CHUNK = 128


def remote(src, dst, send_sem, recv_sem, device_id):
    return pltpu.make_async_remote_copy(
        src_ref=src, dst_ref=dst, send_sem=send_sem, recv_sem=recv_sem, device_id=device_id, device_id_type=MESH_ID
    )


def sp_peers():
    sp = lax.axis_index('sp')
    return sp, sp + 1 - 2 * lax.rem(sp, 2), lax.rem(sp + 2, 4)


def enter(peers):
    barrier = pltpu.get_barrier_semaphore()
    for peer in peers:
        pl.semaphore_signal(barrier, inc=1, device_id=peer, device_id_type=MESH_ID)
    pl.semaphore_wait(barrier, len(peers))


def qkv_kernel(h_hbm, scale_hbm, pos_hbm, w_hbm, kc_hbm, vc_hbm, qkv_ref, k_ref, v_ref,
               h_ref, scale_ref, pos_ref, w0_buf, w1_buf, w2_buf, u_ref, cos_ref, sin_ref,
               i_sem, w_sem, c_sem, a_send, a_recv, b_send, b_recv, f_send, f_recv):
    sp, partner, cross = sp_peers()
    n_seq, d = h_ref.shape
    ins = [pltpu.make_async_copy(src, dst, i_sem.at[i])
           for i, (src, dst) in enumerate(((pos_hbm, pos_ref), (h_hbm, h_ref), (scale_hbm, scale_ref)))]
    for copy in ins:
        copy.start()
    bufs = (w0_buf, w1_buf, w2_buf)
    width = sum(buf.shape[1] for buf in bufs)
    pieces = w_sem.shape[1]
    depth = d // pieces
    w_copies, first = [], 0
    for g, buf in enumerate(bufs):
        col = pl.multiple_of(sp * width + first, HD)
        first += buf.shape[1]

        def w_copy(i, g=g, buf=buf, col=col):
            rows = pl.ds(pl.multiple_of(i * depth, depth), depth)
            return pltpu.make_async_copy(w_hbm.at[rows, pl.ds(col, buf.shape[1])], buf.at[rows], w_sem.at[g, i])

        lax.fori_loop(0, pieces, lambda i, carry, w_copy=w_copy: (w_copy(i).start(), carry)[1], 0)
        w_copies.append([w_copy(i) for i in range(pieces)])
    enter([{'sp': partner}, {'sp': cross}])

    ins[0].wait()
    row_id = lax.broadcasted_iota(jnp.int32, (n_seq, n_seq), 0)
    col_id = lax.broadcasted_iota(jnp.int32, (n_seq, n_seq), 1)
    pos = jnp.sum(jnp.where(row_id == col_id, pos_ref[...].astype(F32), 0.0), axis=-1, keepdims=True)
    lane = lax.broadcasted_iota(jnp.int32, (n_seq, HD), 1)
    freq = lax.rem(lane, HD // 2).astype(F32)
    angles = pos * jnp.exp(freq * (-2.0 * math.log(500000.0) / HD))
    cos_ref[...] = jnp.cos(angles)
    sin_part = jnp.sin(angles)
    sin_ref[...] = jnp.where(lane < HD // 2, -sin_part, sin_part)

    ins[1].wait()
    tiles = d // HD

    def tile(k):
        return h_ref[:, k * HD:(k + 1) * HD].astype(F32)

    total = tile(0)
    for k in range(1, tiles):
        total += tile(k)
    mean = jnp.sum(total, axis=-1, keepdims=True) * (1.0 / d)
    total = jnp.zeros((n_seq, HD), F32)
    for k in range(tiles):
        centered = tile(k) - mean
        total += centered * centered
    inv = lax.rsqrt(jnp.sum(total, axis=-1, keepdims=True) * (1.0 / d) + 1e-5)
    ins[2].wait()
    scale_rows = scale_ref[...].astype(F32)
    for k in range(tiles):
        u_ref[:, k * HD:(k + 1) * HD] = ((tile(k) - mean) * inv * scale_rows[k:k + 1, :]).astype(BF16)

    cache_copies = [pltpu.make_async_copy(kc_hbm, k_ref, c_sem.at[0]), pltpu.make_async_copy(vc_hbm, v_ref, c_sem.at[1])]
    odd = lax.rem(sp, 2)
    heads = width // HD
    to_cross, to_partner, forward = [], [], []
    j = 0
    for g, buf in enumerate(bufs):
        acc = None
        for i in range(pieces):
            w_copies[g][i].wait()
            rows = slice(i * depth, (i + 1) * depth)
            if g >= 1 and i == 0:
                cache_copies[g - 1].start()
            part = jnp.dot(u_ref[:, rows], buf[rows, :], preferred_element_type=F32)
            acc = part if acc is None else acc + part
        proj = jnp.clip(acc.astype(BF16).astype(F32), -8.0, 8.0)
        n = buf.shape[1] // HD
        for r in range(n):
            val = proj[:, r * HD:(r + 1) * HD]
            rot = (val * cos_ref[...] + pltpu.roll(val, HD // 2, 1) * sin_ref[...]).astype(BF16).astype(F32)
            if j + r == heads - 1:
                rot = jnp.where(odd == 1, val, rot)
            qkv_ref[sp, j + r] = rot
        mine = qkv_ref.at[sp, pl.ds(j, n)]
        theirs = qkv_ref.at[cross, pl.ds(j, n)]
        to_cross.append(remote(mine, mine, a_send.at[g], a_recv.at[g], {'sp': cross}))
        to_partner.append(remote(mine, mine, b_send.at[g], b_recv.at[g], {'sp': partner}))
        forward.append(remote(theirs, theirs, f_send.at[g], f_recv.at[g], {'sp': partner}))
        to_cross[g].start()
        to_partner[g].start()
        j += n
    for g in range(len(bufs)):
        to_cross[g].wait_recv()
        forward[g].start()
    for copy in cache_copies:
        copy.wait()
    for g in range(len(bufs)):
        to_partner[g].wait()
        to_cross[g].wait_send()
        forward[g].wait()


def attention_kernel(pos_ref, qkv_ref, k_ref, v_ref, k_out, v_out, acc_ref, stat_ref, q_ref, s_ref, p_ref, out_sem):
    n_seq, rows, _ = k_ref.shape
    seq_local = rows // 2
    group = acc_ref.shape[2]
    base = lax.axis_index('sp') * seq_local
    per_kv = group + 2
    n_q = 2 * group

    tile = 16
    row_id = lax.broadcasted_iota(jnp.int32, (tile, HD), 0)
    at_once = 8

    def patch(i, carry):
        for r in range(at_once):
            b = i * at_once + r
            row = 2 * (pos_ref[b] - base)
            start = pl.multiple_of(jnp.clip(row // tile, 0, rows // tile - 1) * tile, tile)
            off = row - start
            for ref, slot in ((k_ref, group), (v_ref, group + 1)):
                block = ref[b, pl.ds(start, tile), :].astype(F32)
                one = qkv_ref[slot, pl.ds(b, 1), :]
                two = qkv_ref[per_kv + slot, pl.ds(b, 1), :]
                block = jnp.where(row_id == off, one, jnp.where(row_id == off + 1, two, block))
                ref[b, pl.ds(start, tile), :] = block.astype(BF16)
        return carry

    def out_copies(i):
        span = pl.ds(i * at_once, at_once)
        return [pltpu.make_async_copy(src.at[span], dst.at[span], out_sem.at[n, i])
                for n, (src, dst) in enumerate(((k_ref, k_out), (v_ref, v_out)))]

    def patch_and_write(i, carry):
        patch(i, carry)
        for copy in out_copies(i - 1):
            copy.start()
        return carry

    pieces = n_seq // at_once
    patch(0, 0)
    lax.fori_loop(1, pieces, patch_and_write, 0)
    for g in range(2):
        for j in range(group):
            q_ref[pl.ds(g * group + j, n_seq, stride=n_q), :] = qkv_ref[g * per_kv + j]
    for copy in out_copies(pieces - 1):
        copy.start()

    col_id = lax.broadcasted_iota(jnp.int32, (n_q, rows), 1)
    head_id = lax.broadcasted_iota(jnp.int32, (n_q, rows), 0) // group
    col_key = jnp.where(lax.rem(col_id, 2) == head_id, col_id, 1 << 30)
    lane = lax.broadcasted_iota(jnp.int32, (n_q, HD), 1)
    upper = lax.broadcasted_iota(jnp.int32, (2 * n_q, HD), 0) < n_q
    factor = HD ** -0.5 * math.log2(math.e)
    pairs = s_ref.shape[0] // (2 * n_q)
    batch = 2 * pairs

    def score(i):
        for r in range(pairs):
            b = i * batch + 2 * r
            q = q_ref[pl.ds(pl.multiple_of(b * n_q, 2 * n_q), 2 * n_q), :]
            lhs = jnp.concatenate([jnp.where(upper, q, 0.0), jnp.where(upper, 0.0, q)], axis=1).astype(BF16)
            rhs = jnp.concatenate([k_ref[b], k_ref[b + 1]], axis=1)
            out = lax.dot_general(lhs, rhs, (((1,), (1,)), ((), ())), preferred_element_type=F32)
            for e in range(2):
                limit = 2 * (pos_ref[b + e] - base + 1)
                half = out[e * n_q:(e + 1) * n_q] * factor
                s_ref[(2 * r + e) * n_q:(2 * r + e + 1) * n_q, :] = jnp.where(col_key < limit, half, NEG)

    def soften(i, stats):
        for r in range(batch):
            b = i * batch + r
            scores = s_ref[r * n_q:(r + 1) * n_q, :]
            top = jnp.maximum(jnp.max(scores, axis=-1, keepdims=True), FLOOR)
            probs = jnp.exp2(scores - top)
            total = jnp.sum(probs, axis=-1, keepdims=True)
            p_ref[r * n_q:(r + 1) * n_q, :] = probs.astype(BF16)
            stats = jnp.where(lane == b, top, jnp.where(lane == b + n_seq, total, stats))
        return stats

    def weigh(i):
        for r in range(pairs):
            b = i * batch + 2 * r
            rhs = jnp.concatenate([v_ref[b], v_ref[b + 1]], axis=1)
            out = jnp.dot(p_ref[2 * r * n_q:(2 * r + 2) * n_q, :], rhs, preferred_element_type=F32)
            for e in range(2):
                own = out[e * n_q:(e + 1) * n_q, e * HD:(e + 1) * HD]
                acc_ref[0, b + e] = own[:group]
                acc_ref[1, b + e] = own[group:]

    steps = n_seq // batch
    stats = jnp.zeros((n_q, HD), F32)
    score(0)
    stats = soften(0, stats)
    score(1)

    def step(i, stats):
        weigh(i)
        stats = soften(i + 1, stats)
        score(i + 2)
        return stats

    stats = lax.fori_loop(0, steps - 2, step, stats)
    weigh(steps - 2)
    stats = soften(steps - 1, stats)
    weigh(steps - 1)
    stat_ref[0] = stats[:group]
    stat_ref[1] = stats[group:]
    for i in range(pieces):
        for copy in out_copies(i):
            copy.wait()


def project_kernel(h_ref, acc_ref, stat_ref, w_hbm, out_ref, w_buf, d_acc, d_stat, m_acc, m_stat, y_acc, y_stat, att, a_ref,
                   part, e_buf, a_buf, b_buf, tot, y_buf, p1_buf, p2_buf,
                   w_sem, st_send, st_recv, d_send, d_recv, y_send, y_recv, g_send, g_recv,
                   e_send, e_recv, b_send, b_recv, t_send, t_recv, ys, yr, p1s, p1r, p2s, p2r):
    sp, partner, cross = sp_peers()
    core = lax.rem(sp, 2)
    y = sp // 2
    z = lax.axis_index('tp')
    is_hub = (z == 1) | (z == 2)
    end_of_hub = 3 * (z - 1)
    hub_of_end = 1 + z // 2
    other_hub = 3 - z
    width = w_buf.shape[1]
    col = pl.multiple_of(core * width, HD)
    w_copy = pltpu.make_async_copy(w_hbm.at[:, pl.ds(col, width)], w_buf, w_sem)
    w_copy.start()

    barrier = pltpu.get_barrier_semaphore()
    for peer in ({'sp': partner}, {'sp': cross}):
        pl.semaphore_signal(barrier, inc=1, device_id=peer, device_id_type=MESH_ID)

    @pl.when(is_hub)
    def _():
        for peer in ({'tp': end_of_hub}, {'tp': other_hub}):
            pl.semaphore_signal(barrier, inc=1, device_id=peer, device_id_type=MESH_ID)
        pl.semaphore_wait(barrier, 4)

    @pl.when(jnp.logical_not(is_hub))
    def _():
        pl.semaphore_signal(barrier, inc=1, device_id={'tp': hub_of_end}, device_id_type=MESH_ID)
        pl.semaphore_wait(barrier, 3)

    group = stat_ref.shape[1]
    seqs = out_ref.shape[0] // 2
    blocks = y_send.shape[0]
    span = seqs // blocks
    height = span * group
    other = 1 - core
    st_copy = remote(stat_ref.at[other], d_stat, st_send.at[0], st_recv.at[0], {'sp': partner})
    st_copy.start()

    def rows_of(half, i):
        return pl.ds(pl.multiple_of((half * blocks + i) * height, height), height)

    d_copies = []
    for n in range(2 * blocks):
        rows = rows_of(1 - y if n < blocks else y, n % blocks)
        copy = remote(acc_ref.at[other, rows], d_acc.at[rows], d_send.at[n], d_recv.at[n], {'sp': partner})
        copy.start()
        d_copies.append(copy)
    st_copy.wait_recv()
    lane = lax.broadcasted_iota(jnp.int32, (group, HD), 1)

    def weights(s0, s1):
        l0, l1 = pltpu.roll(s0, HD // 2, 1), pltpu.roll(s1, HD // 2, 1)
        top = jnp.maximum(s0, s1)
        e0, e1 = jnp.exp2(s0 - top), jnp.exp2(s1 - top)
        return top, e0, e1, l0 * e0 + l1 * e1

    def lanes_of(half, val):
        return jnp.where(half == 0, val, pltpu.roll(val, HD - seqs, 1))

    top, e0, e1, total = weights(stat_ref[core], d_stat[...])
    m_stat[...] = jnp.where(lane < HD // 2, top, pltpu.roll(total, HD // 2, 1))
    sy_copy = remote(m_stat, y_stat, st_send.at[1], st_recv.at[1], {'sp': cross})
    y_copies = []
    for n in range(2 * blocks):
        half, i = (1 - y if n < blocks else y), n % blocks
        d_copies[n].wait_recv()
        f0, f1 = lanes_of(half, e0), lanes_of(half, e1)
        first = half * seqs * group
        for r in range(span):
            b = i * span + r
            rows = pl.ds(pl.multiple_of(first + b * group, group), group)
            m_acc[rows, :] = acc_ref[core, rows, :] * f0[:, b:b + 1] + d_acc[rows, :] * f1[:, b:b + 1]
        if n == 0:
            sy_copy.start()
        if n < blocks:
            copy = remote(m_acc.at[rows_of(half, i)], y_acc.at[pl.ds(i * height, height)], y_send.at[i], y_recv.at[i], {'sp': cross})
            copy.start()
            y_copies.append(copy)
    sy_copy.wait_recv()
    top, e0, e1, total = weights(m_stat[...], y_stat[...])
    share = 1.0 / jnp.where(lane < HD // 2, total, 1.0)
    e0, e1 = lanes_of(y, e0 * share), lanes_of(y, e1 * share)
    first = y * seqs * group
    g_copies = []
    for i in range(blocks):
        y_copies[i].wait_recv()
        for r in range(span):
            b = i * span + r
            rows = pl.ds(b * group, group)
            mine = m_acc[pl.ds(pl.multiple_of(first + b * group, group), group), :]
            val = mine * e0[:, b:b + 1] + y_acc[rows, :] * e1[:, b:b + 1]
            att[core, rows, :] = val.astype(BF16).astype(F32)
        block = att.at[core, pl.ds(i * height, height)]
        copy = remote(block, block, g_send.at[i], g_recv.at[i], {'sp': partner})
        copy.start()
        g_copies.append(copy)
    for i in range(blocks):
        g_copies[i].wait_recv()
    for g in range(2):
        for j in range(group):
            n = g * group + j
            a_ref[:, n * HD:(n + 1) * HD] = att[g, pl.ds(j, seqs, stride=group), :].astype(BF16)
    w_copy.wait()

    chunks = part.shape[0]
    wide = part.shape[2]

    per_dot = 256 // wide

    def compute(j):
        val = jnp.dot(a_ref[...], w_buf[:, j * 256:(j + 1) * 256], preferred_element_type=F32)
        for n in range(per_dot):
            part[j * per_dot + n] = val[:, n * wide:(n + 1) * wide]

    def emit(half, side, i, ref):
        at = (pl.ds(pl.multiple_of(half * seqs, seqs), seqs), pl.ds(pl.multiple_of(side * width + i * wide, wide), wide))
        out_ref[at] = (h_ref[at].astype(F32) + ref[i]).astype(BF16)

    def e_copy(i):
        return remote(part.at[i], e_buf.at[i], e_send.at[i], e_recv.at[i], {'tp': hub_of_end})

    def b_copy(i):
        return remote(a_buf.at[i], b_buf.at[i], b_send.at[i], b_recv.at[i], {'tp': other_hub})

    def t_copy(i):
        return remote(tot.at[i], tot.at[i], t_send.at[i], t_recv.at[i], {'tp': end_of_hub})

    def y_copy(i):
        return remote(tot.at[i], y_buf.at[i], ys.at[i], yr.at[i], {'sp': cross})

    def p1_copy(i):
        return remote(tot.at[i], p1_buf.at[i], p1s.at[i], p1r.at[i], {'sp': partner})

    def p2_copy(i):
        return remote(y_buf.at[i], p2_buf.at[i], p2s.at[i], p2r.at[i], {'sp': partner})

    def spread(i):
        y_copy(i).start()
        p1_copy(i).start()
        emit(y, core, i, tot)

    def pass_on(i):
        y_copy(i).wait_recv()
        p2_copy(i).start()
        emit(1 - y, core, i, y_buf)

    @pl.when(is_hub)
    def _():
        lag, lag2 = 12, 28
        for j in range(chunks // per_dot):
            compute(j)
        for t in range(chunks + lag2):
            if t < chunks:
                e_copy(t).wait_recv()
                a_buf[t] = part[t] + e_buf[t]
                b_copy(t).start()
            i = t - lag
            if 0 <= i < chunks:
                b_copy(i).wait_recv()
                tot[i] = a_buf[i] + b_buf[i]
                t_copy(i).start()
                spread(i)
            i = t - lag2
            if 0 <= i < chunks:
                pass_on(i)
        for i in range(chunks):
            b_copy(i).wait_send()
            t_copy(i).wait_send()

    @pl.when(jnp.logical_not(is_hub))
    def _():
        lag = 18
        for j in range(chunks // per_dot + 1):
            if j < chunks // per_dot:
                compute(j)
            for n in range(per_dot):
                if j > 0:
                    e_copy((j - 1) * per_dot + n).start()
        for t in range(chunks + lag):
            if t < chunks:
                t_copy(t).wait_recv()
                spread(t)
            i = t - lag
            if 0 <= i < chunks:
                pass_on(i)
        for i in range(chunks):
            e_copy(i).wait_send()

    for i in range(chunks):
        p1_copy(i).wait_recv()
        emit(y, other, i, p1_buf)
        p2_copy(i).wait_recv()
        emit(1 - y, other, i, p2_buf)
    for i in range(chunks):
        y_copy(i).wait_send()
        p1_copy(i).wait_send()
        p2_copy(i).wait_send()
    st_copy.wait_send()
    sy_copy.wait_send()
    for copy in d_copies + y_copies + g_copies:
        copy.wait_send()


def solution(mesh):
    cache_spec = P('dp', 'sp', 'tp', None)
    hbm = pl.BlockSpec(memory_space=pltpu.HBM)
    vmem = pl.BlockSpec(memory_space=pltpu.VMEM)
    smem = pl.BlockSpec(memory_space=pltpu.SMEM)
    dma = pltpu.SemaphoreType.DMA

    def local_step(hidden, norm_scale, w_qkv, w_out, k_cache, v_cache, positions):
        n_seq, seq_local, kv_local, head_dim = k_cache.shape
        d = hidden.shape[1]
        rows = seq_local * kv_local
        heads = w_qkv.shape[1] // head_dim
        group = heads // kv_local - 2
        k_flat = k_cache.reshape(n_seq, rows, head_dim)
        v_flat = v_cache.reshape(n_seq, rows, head_dim)
        share = heads // 4
        in_hbm = [pltpu.with_memory_space_constraint(a, pltpu.HBM)
                  for a in (hidden, norm_scale.reshape(d // head_dim, head_dim), positions.reshape(1, n_seq), w_qkv, k_flat, v_flat)]
        cache_type = pltpu.VMEM((n_seq, rows, head_dim), BF16)
        table = pltpu.VMEM((n_seq, head_dim), F32)
        groups = [2, 2, share - 4]
        qkv, k_vmem, v_vmem = pl.pallas_call(
            qkv_kernel,
            out_shape=[pltpu.VMEM((4, share, n_seq, head_dim), F32), cache_type, cache_type],
            in_specs=[hbm] * 6,
            out_specs=[vmem, vmem, vmem],
            scratch_shapes=[
                pltpu.VMEM((n_seq, d), BF16), pltpu.VMEM((d // head_dim, head_dim), BF16), pltpu.VMEM((1, n_seq), jnp.int32),
                *[pltpu.VMEM((d, n * head_dim), BF16) for n in groups], pltpu.VMEM((n_seq, d), BF16), table, table,
                dma((3,)), dma((3, 2)), dma((2,)), *[dma((3,)) for _ in range(6)],
            ],
            compiler_params=pltpu.CompilerParams(collective_id=0, has_side_effects=True, vmem_limit_bytes=24 << 20),
            name='qkv',
        )(*in_hbm)
        qkv = qkv.reshape(heads, n_seq, head_dim)

        batch = 8
        k_out, v_out, acc, stat = pl.pallas_call(
            attention_kernel,
            out_shape=[
                jax.ShapeDtypeStruct(k_flat.shape, BF16), jax.ShapeDtypeStruct(v_flat.shape, BF16),
                pltpu.VMEM((2, n_seq, group, head_dim), F32), pltpu.VMEM((2, group, head_dim), F32),
            ],
            in_specs=[smem, vmem, vmem, vmem],
            out_specs=[hbm, hbm, vmem, vmem],
            scratch_shapes=[
                pltpu.VMEM((n_seq * 2 * group, head_dim), F32), pltpu.VMEM((batch * 2 * group, rows), F32),
                pltpu.VMEM((batch * 2 * group, rows), BF16), dma((2, 8)),
            ],
            compiler_params=pltpu.CompilerParams(vmem_limit_bytes=16 << 20),
            name='attention',
        )(positions, qkv, k_vmem, v_vmem)
        acc = acc.reshape(2, n_seq * group, head_dim)

        width = d // 2
        depth = w_out.shape[0]
        wide = CHUNK
        chunks = width // wide
        blocks = 4
        seqs = n_seq // 2
        slot = pltpu.VMEM((chunks, seqs, wide), F32)
        whole = pltpu.VMEM((n_seq * group, head_dim), F32)
        half = pltpu.VMEM((seqs * group, head_dim), F32)
        tile = pltpu.VMEM((group, head_dim), F32)
        h_out = pl.pallas_call(
            project_kernel,
            out_shape=jax.ShapeDtypeStruct((n_seq, d), BF16),
            in_specs=[vmem, vmem, vmem, hbm],
            out_specs=vmem,
            scratch_shapes=[
                pltpu.VMEM((depth, width), BF16), whole, tile, whole, tile, half, tile,
                pltpu.VMEM((2, seqs * group, head_dim), F32), pltpu.VMEM((seqs, depth), BF16),
                slot, slot, slot, slot, slot, slot, slot, slot,
                dma(()), dma((2,)), dma((2,)), dma((2 * blocks,)), dma((2 * blocks,)), *[dma((blocks,)) for _ in range(4)],
                *[dma((chunks,)) for _ in range(12)],
            ],
            compiler_params=pltpu.CompilerParams(collective_id=1, has_side_effects=True, vmem_limit_bytes=40 << 20),
            name='project',
        )(hidden, acc, stat, pltpu.with_memory_space_constraint(w_out, pltpu.HBM))
        return h_out, k_out.reshape(k_cache.shape), v_out.reshape(v_cache.shape)

    return jax.shard_map(
        local_step,
        mesh=mesh,
        in_specs=(P('dp', None), P(None), P(None, 'tp'), P('tp', None), cache_spec, cache_spec, P('dp')),
        out_specs=(P('dp', None), cache_spec, cache_spec),
        check_vma=False,
    )
```

```python
import math
import jax
import jax.numpy as jnp
from jax import lax
from jax.experimental import pallas as pl
from jax.experimental.pallas import tpu as pltpu
from jax.sharding import PartitionSpec as P

F32 = jnp.float32
BF16 = jnp.bfloat16
HD = 128
NEG = -3e38
FLOOR = -1e38
MESH_ID = pl.DeviceIdType.MESH
CHUNK = 128


def remote(src, dst, send_sem, recv_sem, device_id):
    return pltpu.make_async_remote_copy(
        src_ref=src, dst_ref=dst, send_sem=send_sem, recv_sem=recv_sem, device_id=device_id, device_id_type=MESH_ID
    )


def sp_peers():
    sp = lax.axis_index('sp')
    return sp, sp + 1 - 2 * lax.rem(sp, 2), lax.rem(sp + 2, 4)


def enter(peers):
    barrier = pltpu.get_barrier_semaphore()
    for peer in peers:
        pl.semaphore_signal(barrier, inc=1, device_id=peer, device_id_type=MESH_ID)
    pl.semaphore_wait(barrier, len(peers))


def qkv_kernel(h_hbm, scale_hbm, pos_hbm, w_hbm, kc_hbm, vc_hbm, qkv_ref, k_ref, v_ref,
               h_ref, scale_ref, pos_ref, w0_buf, w1_buf, w2_buf, u_ref, cos_ref, sin_ref,
               i_sem, w_sem, c_sem, a_send, a_recv, b_send, b_recv, f_send, f_recv):
    sp, partner, cross = sp_peers()
    n_seq, d = h_ref.shape
    ins = [pltpu.make_async_copy(src, dst, i_sem.at[i])
           for i, (src, dst) in enumerate(((pos_hbm, pos_ref), (h_hbm, h_ref), (scale_hbm, scale_ref)))]
    for copy in ins:
        copy.start()
    bufs = (w0_buf, w1_buf, w2_buf)
    width = sum(buf.shape[1] for buf in bufs)
    pieces = w_sem.shape[1]
    depth = d // pieces
    w_copies, first = [], 0
    for g, buf in enumerate(bufs):
        col = pl.multiple_of(sp * width + first, HD)
        first += buf.shape[1]

        def w_copy(i, g=g, buf=buf, col=col):
            rows = pl.ds(pl.multiple_of(i * depth, depth), depth)
            return pltpu.make_async_copy(w_hbm.at[rows, pl.ds(col, buf.shape[1])], buf.at[rows], w_sem.at[g, i])

        lax.fori_loop(0, pieces, lambda i, carry, w_copy=w_copy: (w_copy(i).start(), carry)[1], 0)
        w_copies.append([w_copy(i) for i in range(pieces)])
    enter([{'sp': partner}, {'sp': cross}])

    ins[0].wait()
    row_id = lax.broadcasted_iota(jnp.int32, (n_seq, n_seq), 0)
    col_id = lax.broadcasted_iota(jnp.int32, (n_seq, n_seq), 1)
    pos = jnp.sum(jnp.where(row_id == col_id, pos_ref[...].astype(F32), 0.0), axis=-1, keepdims=True)
    lane = lax.broadcasted_iota(jnp.int32, (n_seq, HD), 1)
    freq = lax.rem(lane, HD // 2).astype(F32)
    angles = pos * jnp.exp(freq * (-2.0 * math.log(500000.0) / HD))
    cos_ref[...] = jnp.cos(angles)
    sin_part = jnp.sin(angles)
    sin_ref[...] = jnp.where(lane < HD // 2, -sin_part, sin_part)

    ins[1].wait()
    tiles = d // HD

    def tile(k):
        return h_ref[:, k * HD:(k + 1) * HD].astype(F32)

    total = tile(0)
    for k in range(1, tiles):
        total += tile(k)
    mean = jnp.sum(total, axis=-1, keepdims=True) * (1.0 / d)
    total = jnp.zeros((n_seq, HD), F32)
    for k in range(tiles):
        centered = tile(k) - mean
        total += centered * centered
    inv = lax.rsqrt(jnp.sum(total, axis=-1, keepdims=True) * (1.0 / d) + 1e-5)
    ins[2].wait()
    scale_rows = scale_ref[...].astype(F32)
    for k in range(tiles):
        u_ref[:, k * HD:(k + 1) * HD] = ((tile(k) - mean) * inv * scale_rows[k:k + 1, :]).astype(BF16)

    cache_copies = [pltpu.make_async_copy(kc_hbm, k_ref, c_sem.at[0]), pltpu.make_async_copy(vc_hbm, v_ref, c_sem.at[1])]
    odd = lax.rem(sp, 2)
    heads = width // HD
    to_cross, to_partner, forward = [], [], []
    j = 0
    for g, buf in enumerate(bufs):
        acc = None
        for i in range(pieces):
            w_copies[g][i].wait()
            rows = slice(i * depth, (i + 1) * depth)
            if g >= 1 and i == 0:
                cache_copies[g - 1].start()
            part = jnp.dot(u_ref[:, rows], buf[rows, :], preferred_element_type=F32)
            acc = part if acc is None else acc + part
        proj = jnp.clip(acc.astype(BF16).astype(F32), -8.0, 8.0)
        n = buf.shape[1] // HD
        for r in range(n):
            val = proj[:, r * HD:(r + 1) * HD]
            rot = (val * cos_ref[...] + pltpu.roll(val, HD // 2, 1) * sin_ref[...]).astype(BF16).astype(F32)
            if j + r == heads - 1:
                rot = jnp.where(odd == 1, val, rot)
            qkv_ref[sp, j + r] = rot
        mine = qkv_ref.at[sp, pl.ds(j, n)]
        theirs = qkv_ref.at[cross, pl.ds(j, n)]
        to_cross.append(remote(mine, mine, a_send.at[g], a_recv.at[g], {'sp': cross}))
        to_partner.append(remote(mine, mine, b_send.at[g], b_recv.at[g], {'sp': partner}))
        forward.append(remote(theirs, theirs, f_send.at[g], f_recv.at[g], {'sp': partner}))
        to_cross[g].start()
        to_partner[g].start()
        j += n
    for g in range(len(bufs)):
        to_cross[g].wait_recv()
        forward[g].start()
    for copy in cache_copies:
        copy.wait()
    for g in range(len(bufs)):
        to_partner[g].wait()
        to_cross[g].wait_send()
        forward[g].wait()


def attention_kernel(pos_ref, qkv_ref, k_ref, v_ref, k_out, v_out, acc_ref, stat_ref, q_ref, s_ref, p_ref, out_sem):
    n_seq, rows, _ = k_ref.shape
    seq_local = rows // 2
    group = acc_ref.shape[2]
    base = lax.axis_index('sp') * seq_local
    per_kv = group + 2
    n_q = 2 * group

    tile = 16
    row_id = lax.broadcasted_iota(jnp.int32, (tile, HD), 0)
    at_once = 8

    def patch(i, carry):
        for r in range(at_once):
            b = i * at_once + r
            row = 2 * (pos_ref[b] - base)
            start = pl.multiple_of(jnp.clip(row // tile, 0, rows // tile - 1) * tile, tile)
            off = row - start
            for ref, slot in ((k_ref, group), (v_ref, group + 1)):
                block = ref[b, pl.ds(start, tile), :].astype(F32)
                one = qkv_ref[slot, pl.ds(b, 1), :]
                two = qkv_ref[per_kv + slot, pl.ds(b, 1), :]
                block = jnp.where(row_id == off, one, jnp.where(row_id == off + 1, two, block))
                ref[b, pl.ds(start, tile), :] = block.astype(BF16)
        return carry

    def out_copies(i):
        span = pl.ds(i * at_once, at_once)
        return [pltpu.make_async_copy(src.at[span], dst.at[span], out_sem.at[n, i])
                for n, (src, dst) in enumerate(((k_ref, k_out), (v_ref, v_out)))]

    def patch_and_write(i, carry):
        patch(i, carry)
        for copy in out_copies(i - 1):
            copy.start()
        return carry

    pieces = n_seq // at_once
    patch(0, 0)
    lax.fori_loop(1, pieces, patch_and_write, 0)
    for g in range(2):
        for j in range(group):
            q_ref[pl.ds(g * group + j, n_seq, stride=n_q), :] = qkv_ref[g * per_kv + j]
    for copy in out_copies(pieces - 1):
        copy.start()

    col_id = lax.broadcasted_iota(jnp.int32, (n_q, rows), 1)
    head_id = lax.broadcasted_iota(jnp.int32, (n_q, rows), 0) // group
    col_key = jnp.where(lax.rem(col_id, 2) == head_id, col_id, 1 << 30)
    lane = lax.broadcasted_iota(jnp.int32, (n_q, HD), 1)
    upper = lax.broadcasted_iota(jnp.int32, (2 * n_q, HD), 0) < n_q
    factor = HD ** -0.5 * math.log2(math.e)
    pairs = s_ref.shape[0] // (2 * n_q)
    batch = 2 * pairs

    def score(i):
        for r in range(pairs):
            b = i * batch + 2 * r
            q = q_ref[pl.ds(pl.multiple_of(b * n_q, 2 * n_q), 2 * n_q), :]
            lhs = jnp.concatenate([jnp.where(upper, q, 0.0), jnp.where(upper, 0.0, q)], axis=1).astype(BF16)
            rhs = jnp.concatenate([k_ref[b], k_ref[b + 1]], axis=1)
            out = lax.dot_general(lhs, rhs, (((1,), (1,)), ((), ())), preferred_element_type=F32)
            for e in range(2):
                limit = 2 * (pos_ref[b + e] - base + 1)
                half = out[e * n_q:(e + 1) * n_q] * factor
                s_ref[(2 * r + e) * n_q:(2 * r + e + 1) * n_q, :] = jnp.where(col_key < limit, half, NEG)

    def soften(i, stats):
        for r in range(batch):
            b = i * batch + r
            scores = s_ref[r * n_q:(r + 1) * n_q, :]
            top = jnp.maximum(jnp.max(scores, axis=-1, keepdims=True), FLOOR)
            probs = jnp.exp2(scores - top)
            total = jnp.sum(probs, axis=-1, keepdims=True)
            p_ref[r * n_q:(r + 1) * n_q, :] = probs.astype(BF16)
            stats = jnp.where(lane == b, top, jnp.where(lane == b + n_seq, total, stats))
        return stats

    def weigh(i):
        for r in range(pairs):
            b = i * batch + 2 * r
            rhs = jnp.concatenate([v_ref[b], v_ref[b + 1]], axis=1)
            out = jnp.dot(p_ref[2 * r * n_q:(2 * r + 2) * n_q, :], rhs, preferred_element_type=F32)
            for e in range(2):
                own = out[e * n_q:(e + 1) * n_q, e * HD:(e + 1) * HD]
                acc_ref[0, b + e] = own[:group]
                acc_ref[1, b + e] = own[group:]

    steps = n_seq // batch
    stats = jnp.zeros((n_q, HD), F32)
    score(0)
    stats = soften(0, stats)
    score(1)

    def step(i, stats):
        weigh(i)
        stats = soften(i + 1, stats)
        score(i + 2)
        return stats

    stats = lax.fori_loop(0, steps - 2, step, stats)
    weigh(steps - 2)
    stats = soften(steps - 1, stats)
    weigh(steps - 1)
    stat_ref[0] = stats[:group]
    stat_ref[1] = stats[group:]
    for i in range(pieces):
        for copy in out_copies(i):
            copy.wait()


def project_kernel(h_ref, acc_ref, stat_ref, w_hbm, out_ref, w_buf, d_acc, d_stat, m_acc, m_stat, y_acc, y_stat, att, a_ref,
                   part, e_buf, a_buf, b_buf, tot, y_buf, p1_buf, p2_buf,
                   w_sem, st_send, st_recv, d_send, d_recv, y_send, y_recv, g_send, g_recv,
                   e_send, e_recv, b_send, b_recv, t_send, t_recv, ys, yr, p1s, p1r, p2s, p2r):
    sp, partner, cross = sp_peers()
    core = lax.rem(sp, 2)
    y = sp // 2
    z = lax.axis_index('tp')
    is_hub = (z == 1) | (z == 2)
    end_of_hub = 3 * (z - 1)
    hub_of_end = 1 + z // 2
    other_hub = 3 - z
    width = w_buf.shape[1]
    col = pl.multiple_of(core * width, HD)
    w_copy = pltpu.make_async_copy(w_hbm.at[:, pl.ds(col, width)], w_buf, w_sem)
    w_copy.start()

    barrier = pltpu.get_barrier_semaphore()
    for peer in ({'sp': partner}, {'sp': cross}):
        pl.semaphore_signal(barrier, inc=1, device_id=peer, device_id_type=MESH_ID)

    @pl.when(is_hub)
    def _():
        for peer in ({'tp': end_of_hub}, {'tp': other_hub}):
            pl.semaphore_signal(barrier, inc=1, device_id=peer, device_id_type=MESH_ID)
        pl.semaphore_wait(barrier, 4)

    @pl.when(jnp.logical_not(is_hub))
    def _():
        pl.semaphore_signal(barrier, inc=1, device_id={'tp': hub_of_end}, device_id_type=MESH_ID)
        pl.semaphore_wait(barrier, 3)

    group = stat_ref.shape[1]
    seqs = out_ref.shape[0] // 2
    blocks = y_send.shape[0]
    span = seqs // blocks
    height = span * group
    other = 1 - core
    st_copy = remote(stat_ref.at[other], d_stat, st_send.at[0], st_recv.at[0], {'sp': partner})
    st_copy.start()

    def rows_of(half, i):
        return pl.ds(pl.multiple_of((half * blocks + i) * height, height), height)

    d_copies = []
    for n in range(2 * blocks):
        rows = rows_of(1 - y if n < blocks else y, n % blocks)
        copy = remote(acc_ref.at[other, rows], d_acc.at[rows], d_send.at[n], d_recv.at[n], {'sp': partner})
        copy.start()
        d_copies.append(copy)
    st_copy.wait_recv()
    lane = lax.broadcasted_iota(jnp.int32, (group, HD), 1)

    def weights(s0, s1):
        l0, l1 = pltpu.roll(s0, HD // 2, 1), pltpu.roll(s1, HD // 2, 1)
        top = jnp.maximum(s0, s1)
        e0, e1 = jnp.exp2(s0 - top), jnp.exp2(s1 - top)
        return top, e0, e1, l0 * e0 + l1 * e1

    def lanes_of(half, val):
        return jnp.where(half == 0, val, pltpu.roll(val, HD - seqs, 1))

    top, e0, e1, total = weights(stat_ref[core], d_stat[...])
    m_stat[...] = jnp.where(lane < HD // 2, top, pltpu.roll(total, HD // 2, 1))
    sy_copy = remote(m_stat, y_stat, st_send.at[1], st_recv.at[1], {'sp': cross})
    y_copies = []
    for n in range(2 * blocks):
        half, i = (1 - y if n < blocks else y), n % blocks
        d_copies[n].wait_recv()
        f0, f1 = lanes_of(half, e0), lanes_of(half, e1)
        first = half * seqs * group
        for r in range(span):
            b = i * span + r
            rows = pl.ds(pl.multiple_of(first + b * group, group), group)
            m_acc[rows, :] = acc_ref[core, rows, :] * f0[:, b:b + 1] + d_acc[rows, :] * f1[:, b:b + 1]
        if n == 0:
            sy_copy.start()
        if n < blocks:
            copy = remote(m_acc.at[rows_of(half, i)], y_acc.at[pl.ds(i * height, height)], y_send.at[i], y_recv.at[i], {'sp': cross})
            copy.start()
            y_copies.append(copy)
    sy_copy.wait_recv()
    top, e0, e1, total = weights(m_stat[...], y_stat[...])
    share = 1.0 / jnp.where(lane < HD // 2, total, 1.0)
    e0, e1 = lanes_of(y, e0 * share), lanes_of(y, e1 * share)
    first = y * seqs * group
    g_copies = []
    for i in range(blocks):
        y_copies[i].wait_recv()
        for r in range(span):
            b = i * span + r
            rows = pl.ds(b * group, group)
            mine = m_acc[pl.ds(pl.multiple_of(first + b * group, group), group), :]
            val = mine * e0[:, b:b + 1] + y_acc[rows, :] * e1[:, b:b + 1]
            att[core, rows, :] = val.astype(BF16).astype(F32)
        block = att.at[core, pl.ds(i * height, height)]
        copy = remote(block, block, g_send.at[i], g_recv.at[i], {'sp': partner})
        copy.start()
        g_copies.append(copy)
    for i in range(blocks):
        g_copies[i].wait_recv()
    for g in range(2):
        for j in range(group):
            n = g * group + j
            a_ref[:, n * HD:(n + 1) * HD] = att[g, pl.ds(j, seqs, stride=group), :].astype(BF16)
    w_copy.wait()

    chunks = part.shape[0]
    wide = part.shape[2]

    per_dot = 256 // wide

    def compute(j):
        val = jnp.dot(a_ref[...], w_buf[:, j * 256:(j + 1) * 256], preferred_element_type=F32)
        for n in range(per_dot):
            part[j * per_dot + n] = val[:, n * wide:(n + 1) * wide]

    def emit(half, side, i, ref):
        at = (pl.ds(pl.multiple_of(half * seqs, seqs), seqs), pl.ds(pl.multiple_of(side * width + i * wide, wide), wide))
        out_ref[at] = (h_ref[at].astype(F32) + ref[i]).astype(BF16)

    def e_copy(i):
        return remote(part.at[i], e_buf.at[i], e_send.at[i], e_recv.at[i], {'tp': hub_of_end})

    def b_copy(i):
        return remote(a_buf.at[i], b_buf.at[i], b_send.at[i], b_recv.at[i], {'tp': other_hub})

    def t_copy(i):
        return remote(tot.at[i], tot.at[i], t_send.at[i], t_recv.at[i], {'tp': end_of_hub})

    def y_copy(i):
        return remote(tot.at[i], y_buf.at[i], ys.at[i], yr.at[i], {'sp': cross})

    def p1_copy(i):
        return remote(tot.at[i], p1_buf.at[i], p1s.at[i], p1r.at[i], {'sp': partner})

    def p2_copy(i):
        return remote(y_buf.at[i], p2_buf.at[i], p2s.at[i], p2r.at[i], {'sp': partner})

    def spread(i):
        y_copy(i).start()
        p1_copy(i).start()
        emit(y, core, i, tot)

    def pass_on(i):
        y_copy(i).wait_recv()
        p2_copy(i).start()
        emit(1 - y, core, i, y_buf)

    @pl.when(is_hub)
    def _():
        lag, lag2 = 4, 10
        for j in range(chunks // per_dot):
            compute(j)
        for t in range(chunks + lag2):
            if t < chunks:
                e_copy(t).wait_recv()
                a_buf[t] = part[t] + e_buf[t]
                b_copy(t).start()
            i = t - lag
            if 0 <= i < chunks:
                b_copy(i).wait_recv()
                tot[i] = a_buf[i] + b_buf[i]
                t_copy(i).start()
                spread(i)
            i = t - lag2
            if 0 <= i < chunks:
                pass_on(i)
        for i in range(chunks):
            b_copy(i).wait_send()
            t_copy(i).wait_send()

    @pl.when(jnp.logical_not(is_hub))
    def _():
        lag = 6
        for j in range(chunks // per_dot + 1):
            if j < chunks // per_dot:
                compute(j)
            for n in range(per_dot):
                if j > 0:
                    e_copy((j - 1) * per_dot + n).start()
        for t in range(chunks + lag):
            if t < chunks:
                t_copy(t).wait_recv()
                spread(t)
            i = t - lag
            if 0 <= i < chunks:
                pass_on(i)
        for i in range(chunks):
            e_copy(i).wait_send()

    for i in range(chunks):
        p1_copy(i).wait_recv()
        emit(y, other, i, p1_buf)
        p2_copy(i).wait_recv()
        emit(1 - y, other, i, p2_buf)
    for i in range(chunks):
        y_copy(i).wait_send()
        p1_copy(i).wait_send()
        p2_copy(i).wait_send()
    st_copy.wait_send()
    sy_copy.wait_send()
    for copy in d_copies + y_copies + g_copies:
        copy.wait_send()


def solution(mesh):
    cache_spec = P('dp', 'sp', 'tp', None)
    hbm = pl.BlockSpec(memory_space=pltpu.HBM)
    vmem = pl.BlockSpec(memory_space=pltpu.VMEM)
    smem = pl.BlockSpec(memory_space=pltpu.SMEM)
    dma = pltpu.SemaphoreType.DMA

    def local_step(hidden, norm_scale, w_qkv, w_out, k_cache, v_cache, positions):
        n_seq, seq_local, kv_local, head_dim = k_cache.shape
        d = hidden.shape[1]
        rows = seq_local * kv_local
        heads = w_qkv.shape[1] // head_dim
        group = heads // kv_local - 2
        k_flat = k_cache.reshape(n_seq, rows, head_dim)
        v_flat = v_cache.reshape(n_seq, rows, head_dim)
        share = heads // 4
        in_hbm = [pltpu.with_memory_space_constraint(a, pltpu.HBM)
                  for a in (hidden, norm_scale.reshape(d // head_dim, head_dim), positions.reshape(1, n_seq), w_qkv, k_flat, v_flat)]
        cache_type = pltpu.VMEM((n_seq, rows, head_dim), BF16)
        table = pltpu.VMEM((n_seq, head_dim), F32)
        groups = [2, 2, share - 4]
        qkv, k_vmem, v_vmem = pl.pallas_call(
            qkv_kernel,
            out_shape=[pltpu.VMEM((4, share, n_seq, head_dim), F32), cache_type, cache_type],
            in_specs=[hbm] * 6,
            out_specs=[vmem, vmem, vmem],
            scratch_shapes=[
                pltpu.VMEM((n_seq, d), BF16), pltpu.VMEM((d // head_dim, head_dim), BF16), pltpu.VMEM((1, n_seq), jnp.int32),
                *[pltpu.VMEM((d, n * head_dim), BF16) for n in groups], pltpu.VMEM((n_seq, d), BF16), table, table,
                dma((3,)), dma((3, 2)), dma((2,)), *[dma((3,)) for _ in range(6)],
            ],
            compiler_params=pltpu.CompilerParams(collective_id=0, has_side_effects=True, vmem_limit_bytes=24 << 20),
            name='qkv',
        )(*in_hbm)
        qkv = qkv.reshape(heads, n_seq, head_dim)

        batch = 8
        k_out, v_out, acc, stat = pl.pallas_call(
            attention_kernel,
            out_shape=[
                jax.ShapeDtypeStruct(k_flat.shape, BF16), jax.ShapeDtypeStruct(v_flat.shape, BF16),
                pltpu.VMEM((2, n_seq, group, head_dim), F32), pltpu.VMEM((2, group, head_dim), F32),
            ],
            in_specs=[smem, vmem, vmem, vmem],
            out_specs=[hbm, hbm, vmem, vmem],
            scratch_shapes=[
                pltpu.VMEM((n_seq * 2 * group, head_dim), F32), pltpu.VMEM((batch * 2 * group, rows), F32),
                pltpu.VMEM((batch * 2 * group, rows), BF16), dma((2, 8)),
            ],
            compiler_params=pltpu.CompilerParams(vmem_limit_bytes=16 << 20),
            name='attention',
        )(positions, qkv, k_vmem, v_vmem)
        acc = acc.reshape(2, n_seq * group, head_dim)

        width = d // 2
        depth = w_out.shape[0]
        wide = 2 * CHUNK
        chunks = width // wide
        blocks = 4
        seqs = n_seq // 2
        slot = pltpu.VMEM((chunks, seqs, wide), F32)
        whole = pltpu.VMEM((n_seq * group, head_dim), F32)
        half = pltpu.VMEM((seqs * group, head_dim), F32)
        tile = pltpu.VMEM((group, head_dim), F32)
        h_out = pl.pallas_call(
            project_kernel,
            out_shape=jax.ShapeDtypeStruct((n_seq, d), BF16),
            in_specs=[vmem, vmem, vmem, hbm],
            out_specs=vmem,
            scratch_shapes=[
                pltpu.VMEM((depth, width), BF16), whole, tile, whole, tile, half, tile,
                pltpu.VMEM((2, seqs * group, head_dim), F32), pltpu.VMEM((seqs, depth), BF16),
                slot, slot, slot, slot, slot, slot, slot, slot,
                dma(()), dma((2,)), dma((2,)), dma((2 * blocks,)), dma((2 * blocks,)), *[dma((blocks,)) for _ in range(4)],
                *[dma((chunks,)) for _ in range(12)],
            ],
            compiler_params=pltpu.CompilerParams(collective_id=1, has_side_effects=True, vmem_limit_bytes=40 << 20),
            name='project',
        )(hidden, acc, stat, pltpu.with_memory_space_constraint(w_out, pltpu.HBM))
        return h_out, k_out.reshape(k_cache.shape), v_out.reshape(v_cache.shape)

    return jax.shard_map(
        local_step,
        mesh=mesh,
        in_specs=(P('dp', None), P(None), P(None, 'tp'), P('tp', None), cache_spec, cache_spec, P('dp')),
        out_specs=(P('dp', None), cache_spec, cache_spec),
        check_vma=False,
    )
```
